32 devices in a mesh: frames: 8 (over z, x), rows: 4 (over y, core).
Axes of the slice: x: 2, y: 2, z: 4, core: 2. Of those that a mesh axis runs over, the one named last changes fastest.
Arguments:
- fmap: bfloat16 [16, 12, 64, 128], P('frames', 'rows'), may hold values from -6 to 6
- context: bfloat16 [16, 12, 64, 128], P('frames', 'rows'), may hold values from -6 to 6
- pairs: int32 [32, 3], replicated, may hold values from 0 to 15, as said below
- w_corr: bfloat16 [49, 128], replicated, may hold values from -0.875 to 0.875
- w_zr: bfloat16 [256, 256], replicated, may hold values from -0.375 to 0.375
- w_q: bfloat16 [9, 256, 128], replicated, may hold values from -0.125 to 0.125
- w_msg: bfloat16 [128, 256], replicated, may hold values from -0.5 to 0.5
- w_res: bfloat16 [9, 128, 128], replicated, may hold values from -0.1875 to 0.1875
Outputs:
- state: bfloat16 [16, 12, 64, 128], P('frames', 'rows')
The draws below stay inside these ranges and needn't reach their ends.
Inputs may be any that keep to these rules, and one draw needn't show every extreme that they name: Source and target differ. With dev(f) = f // 2, the source's dev, the target's dev and the owner differ pairwise by at most one. No owner holds more than 8 pairs, and some owner holds exactly 8.
All inputs are finite; a program needn't handle non-finite values.
Results may differ from the reference program's by a relative error of at most 0.01.
Values may be sent and summed in bfloat16 or wider, within the bound.
A program may use at most 64 MiB of HBM per device.

```python
import jax
import jax.numpy as jnp

CHANNELS = 128
IMG_WIDTH = 64
FRAME_DEV = 2
PAIR_DEV = 4
RADIUS = 3
ROUNDS = 2
FRAMES = 16
IMG_HEIGHT = 12
PAIR_TOTAL = 32
N_FRAMES = 8


def draw_pairs(key, part):
    keys = jax.random.split(jax.random.fold_in(key, 71), 9)
    halves = N_FRAMES // 2
    capacity = 2 * PAIR_DEV
    loads = jax.random.randint(keys[0], (halves,), 0, capacity + 1).astype(jnp.int32)
    forced = jax.random.randint(keys[1], (), 1, halves - 1).astype(jnp.int32)
    half_ids = jnp.arange(halves, dtype=jnp.int32)
    loads = jnp.where(half_ids == forced, capacity, loads).astype(jnp.int32)
    flips = jax.random.randint(keys[2], (halves,), 0, 2).astype(jnp.int32)
    evens = jnp.where(flips == 1, loads, capacity - loads).astype(jnp.int32)
    evens = jnp.where(half_ids == halves - 1, jnp.maximum(evens, 1), evens).astype(jnp.int32)
    evens = jnp.where(half_ids == 0, jnp.minimum(evens, capacity - 1), evens).astype(jnp.int32)
    counts = jnp.stack([evens, capacity - evens], axis=1).reshape(N_FRAMES).astype(jnp.int32)
    ends = jnp.cumsum(counts).astype(jnp.int32)
    positions = jnp.arange(PAIR_TOTAL, dtype=jnp.int32)
    owners = jnp.sum((positions[:, None] >= ends[None, :]).astype(jnp.int32), axis=1).astype(jnp.int32)
    src_step = jax.random.randint(keys[3], (PAIR_TOTAL,), -1, 2).astype(jnp.int32)
    src_dev = jnp.clip(owners + src_step, 0, N_FRAMES - 1).astype(jnp.int32)
    tgt_step = jax.random.randint(keys[4], (PAIR_TOTAL,), -1, 2).astype(jnp.int32)
    picker = jax.random.randint(keys[5], (PAIR_TOTAL,), 0, 2).astype(jnp.int32)
    tgt_dev = jnp.where(src_dev == owners, jnp.clip(owners + tgt_step, 0, N_FRAMES - 1), jnp.where(picker == 0, owners, src_dev)).astype(jnp.int32)
    high_first = ends[N_FRAMES - 3]
    low_first = ends[0]
    src_dev = jnp.where(positions == high_first, N_FRAMES - 2, src_dev).astype(jnp.int32)
    tgt_dev = jnp.where(positions == high_first, N_FRAMES - 1, tgt_dev).astype(jnp.int32)
    src_dev = jnp.where(positions == low_first, 0, src_dev).astype(jnp.int32)
    tgt_dev = jnp.where(positions == low_first, 1, tgt_dev).astype(jnp.int32)
    sources = (src_dev * FRAME_DEV + jax.random.randint(keys[6], (PAIR_TOTAL,), 0, FRAME_DEV)).astype(jnp.int32)
    targets = (tgt_dev * FRAME_DEV + jax.random.randint(keys[7], (PAIR_TOTAL,), 0, FRAME_DEV)).astype(jnp.int32)
    other = (src_dev * FRAME_DEV + (sources % FRAME_DEV + 1) % FRAME_DEV).astype(jnp.int32)
    targets = jnp.where(targets == sources, other, targets).astype(jnp.int32)
    table = jnp.stack([sources, targets, owners], axis=1).astype(jnp.int32)
    order = jax.random.permutation(keys[8], PAIR_TOTAL)
    return jnp.take(table, order, axis=0).astype(jnp.int32)


def shard_levels(rng, dims, shards, least, top_value):
    loudness = 1.0
    for dim, parts in shards:
        steps = jax.random.uniform(jax.random.fold_in(jax.random.fold_in(rng, 6), dim), (parts,), jnp.float32, least / len(shards), top_value / len(shards))
        loudness = loudness * jnp.repeat(jnp.exp(steps), dims[dim] // parts).reshape((-1,) + (1,) * (len(dims) - 1 - dim))
    return loudness


def bell_draw(key, extent, deviation, reach, shards=(), kind=jnp.bfloat16):
    array = jax.random.normal(key, extent, jnp.float32) * deviation
    if len(shards) > 0:
        array = shard_levels(key, extent, shards, -0.22, 0.18) * array
    return jnp.clip(array, min=-reach, max=reach).astype(kind)


def setup_inputs(seed: int = 0) -> dict:
    arg_keys = jax.random.split(jax.random.key(seed), 9)
    return {
        "fmap": bell_draw(arg_keys[0], (FRAMES, IMG_HEIGHT, IMG_WIDTH, CHANNELS), 1.0, 6.0, ((0, 8), (1, 4))),
        "context": bell_draw(arg_keys[1], (FRAMES, IMG_HEIGHT, IMG_WIDTH, CHANNELS), 1.0, 6.0, ((0, 8), (1, 4))),
        "pairs": draw_pairs(jax.random.fold_in(arg_keys[8], 71), 0),
        "w_corr": bell_draw(arg_keys[3], ((2 * RADIUS + 1) ** 2, CHANNELS), ((2 * RADIUS + 1) ** 2) ** -0.5, 0.875),
        "w_zr": bell_draw(arg_keys[4], (2 * CHANNELS, 2 * CHANNELS), (2 * CHANNELS) ** -0.5, 0.375),
        "w_q": bell_draw(arg_keys[5], (9, 2 * CHANNELS, CHANNELS), (18 * CHANNELS) ** -0.5, 0.125),
        "w_msg": bell_draw(arg_keys[6], (CHANNELS, 2 * CHANNELS), CHANNELS ** -0.5, 0.5),
        "w_res": bell_draw(arg_keys[7], (9, CHANNELS, CHANNELS), (9 * CHANNELS) ** -0.5, 0.1875),
    }


def conv_three(padded, kernel, height, width):
    count = padded.shape[0]
    cin = padded.shape[-1]
    total = None
    for row_off in range(3):
        for col_off in range(3):
            window = padded[:, row_off:row_off + height, col_off:col_off + width, :].reshape(-1, cin)
            term = jnp.dot(window, kernel[3 * row_off + col_off], preferred_element_type=jnp.float32)
            total = term if total is None else total + term
    return total.reshape(count, height, width, -1)


def pad_both(field, amount):
    return jnp.pad(field, ((0, 0), (amount, amount), (amount, amount), (0, 0)))


def reference(fmap, context, pairs, w_corr, w_zr, w_q, w_msg, w_res):
    sources = pairs[:, 0].astype(jnp.int32)
    targets = pairs[:, 1].astype(jnp.int32)
    height = fmap.shape[1]
    width = fmap.shape[2]
    chans = fmap.shape[3]
    span = 2 * RADIUS + 1
    src_feat = jnp.take(fmap, sources, axis=0).astype(jnp.float32)
    tgt_pad = pad_both(jnp.take(fmap, targets, axis=0), RADIUS)
    columns = []
    for row_off in range(span):
        for col_off in range(span):
            moved = tgt_pad[:, row_off:row_off + height, col_off:col_off + width, :].astype(jnp.float32)
            columns.append(jnp.einsum('pyxc,pyxc->pyx', src_feat, moved))
    scale = 1.0 / (chans ** 0.5)
    corr = (jnp.stack(columns, axis=-1) * scale).astype(jnp.bfloat16)
    motion = jax.nn.relu(jnp.dot(corr.reshape(-1, span * span), w_corr, preferred_element_type=jnp.float32))
    motion = motion.astype(jnp.bfloat16).reshape(-1, height, width, chans)
    state = context
    hidden = None
    for sweep in range(ROUNDS):
        ctx_src = jnp.take(state, sources, axis=0).astype(jnp.float32)
        if sweep == 0:
            hidden = jnp.tanh(ctx_src)
        xin = (motion.astype(jnp.float32) + ctx_src).astype(jnp.bfloat16)
        joined = jnp.concatenate([hidden.astype(jnp.bfloat16), xin], axis=-1)
        gates = jax.nn.sigmoid(jnp.dot(joined.reshape(-1, 2 * chans), w_zr, preferred_element_type=jnp.float32))
        gates = gates.reshape(-1, height, width, 2 * chans)
        update_gate = gates[..., :chans]
        reset_gate = gates[..., chans:]
        qin = jnp.concatenate([(reset_gate * hidden).astype(jnp.bfloat16), xin], axis=-1)
        candidate = jnp.tanh(conv_three(pad_both(qin, 1), w_q, height, width))
        hidden = (1.0 - update_gate) * hidden + update_gate * candidate
        messages = jnp.dot(hidden.astype(jnp.bfloat16).reshape(-1, chans), w_msg, preferred_element_type=jnp.float32)
        messages = messages.astype(jnp.bfloat16).reshape(-1, height, width, 2 * chans)
        incoming = jax.ops.segment_sum(messages[..., :chans].astype(jnp.float32), sources, num_segments=FRAMES)
        incoming = incoming + jax.ops.segment_sum(messages[..., chans:].astype(jnp.float32), targets, num_segments=FRAMES)
        update = jax.nn.relu(incoming).astype(jnp.bfloat16)
        state = (state.astype(jnp.float32) + conv_three(pad_both(update, 1), w_res, height, width)).astype(jnp.bfloat16)
    return state
```

```python
import functools

import jax
import jax.numpy as jnp
from jax import lax
from jax.experimental import pallas as pl
from jax.experimental.pallas import tpu as pltpu
from jax.sharding import PartitionSpec as P

RADIUS = 3
ROUNDS = 2
LANES = 128
SPAN = 2 * RADIUS + 1
MESH = pl.DeviceIdType.MESH
F32 = jnp.float32
BF16 = jnp.bfloat16
LEFT, RIGHT, UP, DOWN = range(4)


def dot(a, b):
    return jnp.dot(a, b, preferred_element_type=F32)


def dot_nt(a, b):
    return lax.dot_general(a, b, (((1,), (1,)), ((), ())), preferred_element_type=F32)


def plan(fd):
    groups = []
    for j in range(fd):
        for way, seat in ((LEFT, j), (RIGHT, 2 * fd + j)):
            groups.append((way, j, [(i, seat) for i in range(fd)]))
    groups.append((None, 0, [(i, fd + j) for j in range(fd) for i in range(fd) if i != j]))
    start = 0
    out = []
    for way, j, members in groups:
        out.append((way, j, start, members))
        start += len(members)
    return out, start


def kernel(
    nf, nr,
    pairs_ref, fmap_ref, ctx_ref, wcorr_ref, wzr_ref, wq_ref, wmsg_ref, wres_ref,
    out_ref,
    fsrc, fwin, st, mot, hid, hh, th, hw0, hw, qbuf, zbuf, asum, bsum,
    msend, mrecv, ubuf, mown,
    wcorr_s, wsel, wzr_s, wq_s, wres_s, wmsg_s, tbl,
    ssem, rsem, lsem,
):
    f = lax.axis_index("frames")
    r = lax.axis_index("rows")
    height, fd, width, chans = fsrc.shape
    npair = pairs_ref.shape[1]
    rows = height * width
    tall = (height + 2) * width
    groups, total_combos = plan(fd)
    has = {LEFT: f > 0, RIGHT: f < nf - 1, UP: r > 0, DOWN: r < nr - 1}
    dev = {LEFT: (f - 1, r), RIGHT: (f + 1, r), UP: (f, r - 1), DOWN: (f, r + 1)}
    back = {LEFT: RIGHT, RIGHT: LEFT, UP: DOWN, DOWN: UP}
    sent = []

    def both(cond, gate):
        return cond if gate is None else jnp.logical_and(cond, gate)

    def rcopy(handle):
        i, way, src, dst, _ = handle
        return pltpu.make_async_remote_copy(
            src_ref=src, dst_ref=dst, send_sem=ssem.at[i], recv_sem=rsem.at[i],
            device_id=dev[way], device_id_type=MESH,
        )

    def push(way, src, dst, gate=None):
        handle = (len(sent), way, src, dst, gate)
        sent.append(handle)

        @pl.when(both(has[way], gate))
        def _():
            rcopy(handle).start()

        return handle

    def arrive(handle):
        @pl.when(both(has[back[handle[1]]], handle[4]))
        def _():
            rcopy(handle).wait_recv()

    own_rows = pl.ds(RADIUS, height)
    middle = pl.ds(fd, fd)
    seat = {RIGHT: 0, LEFT: 2 * fd}

    barrier = pltpu.get_barrier_semaphore()
    count = 0
    for way in (LEFT, RIGHT, UP, DOWN):
        count = count + has[way].astype(jnp.int32)

        @pl.when(has[way])
        def _(way=way):
            pl.semaphore_signal(barrier, inc=1, device_id=dev[way], device_id_type=MESH)

    loads = []

    def load(src, dst):
        copy = pltpu.make_async_copy(src, dst, lsem.at[len(loads)])
        loads.append(copy)
        copy.start()
        return copy

    own_f = [load(fmap_ref.at[i], fsrc.at[:, i]) for i in range(fd)]
    own_c = load(ctx_ref, st.at[0, :, pl.ds(1, height)])
    corr_w = load(wcorr_ref, wcorr_s)
    gate_w = load(wzr_ref, wzr_s)
    late = []
    for k in range(3):
        for j in range(3):
            lanes = pl.ds(j * chans, chans)
            late.append(load(wq_ref.at[3 * k + j], wq_s.at[pl.ds(2 * k * chans, 2 * chans), lanes]))
            late.append(load(wres_ref.at[3 * k + j], wres_s.at[pl.ds(k * chans, chans), lanes]))
    for k in range(2):
        lanes = pl.ds(k * chans, chans)
        late.append(load(wmsg_ref.at[:, lanes], wmsg_s.at[lanes]))

    flip = jnp.where(
        lax.broadcasted_iota(jnp.int32, (width, width), 0)
        + lax.broadcasted_iota(jnp.int32, (width, width), 1)
        == width - 1,
        1.0,
        0.0,
    ).astype(BF16)
    for copy in own_f:
        copy.wait()
    for i in range(fd):
        for y in range(height):
            fwin[fd + i, RADIUS + y] = dot(flip, fsrc[y, i]).astype(BF16)
    pl.semaphore_wait(barrier, count)

    feats = {}
    edge_src = {UP: pl.ds(RADIUS, RADIUS), DOWN: pl.ds(height, RADIUS)}
    edge_dst = {UP: pl.ds(RADIUS + height, RADIUS), DOWN: pl.ds(0, RADIUS)}
    own_edges = []
    for j in range(fd):
        for way in (RIGHT, LEFT):
            feats[way, j] = push(
                way, fwin.at[fd + j, own_rows], fwin.at[seat[way] + j, own_rows]
            )
        if j == 0:
            own_edges = [
                push(way, fwin.at[middle, edge_src[way]], fwin.at[middle, edge_dst[way]])
                for way in (UP, DOWN)
            ]
    line_src = {UP: 1, DOWN: height}
    line_dst = {UP: height + 1, DOWN: 0}
    own_c.wait()
    ctx_edges = [
        push(way, st.at[0, :, line_src[way]], st.at[0, :, line_dst[way]]) for way in (UP, DOWN)
    ]

    fwin[:, 2 * RADIUS + height] = jnp.zeros((fwin.shape[0],) + fwin.shape[2:], BF16)
    for way, edge in ((UP, r == 0), (DOWN, r == nr - 1)):
        @pl.when(edge)
        def _(way=way):
            outside = back[way]
            fwin[:, edge_dst[outside]] = jnp.zeros(
                (fwin.shape[0], RADIUS, width, chans), BF16
            )
            line = line_dst[outside]
            mot[:, line] = jnp.zeros((total_combos, width, chans), BF16)
            hh[:, :, line] = jnp.zeros(hh.shape[:2] + (width, chans), BF16)
            st[0, :, line] = jnp.zeros((fd, width, chans), BF16)
            first = 0 if way == UP else height + 2
            ubuf[:, :, first : first + 2] = jnp.zeros((ROUNDS, fd, 2, width, chans), BF16)

    for way, edge in ((RIGHT, f == 0), (LEFT, f == nf - 1)):
        @pl.when(edge)
        def _(way=way):
            fwin[seat[way] : seat[way] + fd] = jnp.zeros((fd,) + fwin.shape[1:], BF16)
            for k in range(ROUNDS):
                mrecv[k, way] = jnp.zeros((fd, rows, chans), BF16)

    window = 3 * fd
    base_s = f * fd
    base_t = (f - 1) * fd
    codes = [i * window + j for _, _, _, members in groups for i, j in members]

    def tally(p, counts):
        i = pairs_ref[0, p] - base_s
        j = pairs_ref[1, p] - base_t
        own = jnp.logical_and(i >= 0, i < fd)
        code = jnp.where(own, i * window + j, -1)
        return tuple(v + (code == c).astype(jnp.int32) for v, c in zip(counts, codes))

    counts = lax.fori_loop(0, npair, tally, (jnp.int32(0),) * total_combos)
    for c in range(total_combos):
        tbl[c] = counts[c]

    def times(c):
        return tbl[c].astype(F32)

    per = LANES // width
    tiles = (SPAN + per - 1) // per
    depth = tiles * LANES
    origin = width - 1 - RADIUS

    def place(lane):
        spot = lax.rem(lane + (LANES - origin), LANES)
        return lax.div(spot, width), (SPAN - 1) - lax.rem(spot, width)

    corr_w.wait()
    line = lax.broadcasted_iota(jnp.int32, (depth, wcorr_s.shape[0]), 0)
    col = lax.broadcasted_iota(jnp.int32, (depth, wcorr_s.shape[0]), 1)
    half, b_off = place(lax.rem(line, LANES))
    a_off = lax.div(line, LANES) * per + half
    take = jnp.logical_and(b_off >= 0, a_off < SPAN)
    index = jnp.where(take, a_off * SPAN + b_off, -1)
    wsel[...] = dot(jnp.where(index == col, 1.0, 0.0).astype(BF16), wcorr_s[...]).astype(BF16)

    xs = lax.broadcasted_iota(jnp.int32, (width, LANES), 0)
    _, bs = place(lax.broadcasted_iota(jnp.int32, (width, LANES), 1))
    inside = jnp.logical_and(xs + bs >= RADIUS, xs + bs < width + RADIUS)
    inside = jnp.logical_and(inside, bs >= 0)
    scale = 1.0 / chans**0.5

    def banded(g):
        pieces = []
        for q in range(tiles):
            piece = pltpu.roll(g[:, q * LANES : (q + 1) * LANES], 0, 1, stride=1, stride_axis=0)
            pieces.append(jnp.where(inside, piece, 0.0).astype(BF16))
        return jnp.concatenate(pieces, axis=1)

    def correlate(group):
        way, _, start, members = group
        lines = [[] for _ in members]
        for y in range(height):
            if way is None:
                for n, (i, j) in enumerate(members):
                    b = fwin[j, y : y + tiles * per].reshape(tiles * per * width, chans)
                    lines[n].append(banded(dot_nt(fsrc[y, i], b)))
            else:
                j = members[0][1]
                b = fwin[j, y : y + tiles * per].reshape(tiles * per * width, chans)
                g = dot_nt(fsrc[y].reshape(fd * width, chans), b)
                for n in range(fd):
                    lines[n].append(banded(g[n * width : (n + 1) * width]))
        corr = jnp.concatenate([part for each in lines for part in each], axis=0)
        moved = jnp.maximum(dot(corr, wsel[...]) * scale, 0.0).astype(BF16)
        n = len(members)
        mot[start : start + n, 1 : height + 1] = moved.reshape(n, height, width, chans)
        span = pl.ds(start, n)
        return [
            push(side, mot.at[span, line_src[side]], mot.at[span, line_dst[side]])
            for side in (UP, DOWN)
        ]

    for handle in own_edges:
        arrive(handle)
    mot_edges = {len(groups) - 1: correlate(groups[-1])}
    relays = {}
    for j in range(fd):
        for way in (RIGHT, LEFT):
            arrive(feats[way, j])
            spot = seat[way] + j
            relays[spot] = [
                push(
                    side, fwin.at[spot, edge_src[side]], fwin.at[spot, edge_dst[side]],
                    gate=has[back[way]],
                )
                for side in (UP, DOWN)
            ]
    for handle in ctx_edges:
        arrive(handle)
    gate_w.wait()
    for i in range(fd):
        first = jnp.tanh(st[0, i].reshape(tall, chans).astype(F32))
        th[i] = first
        hw0[i] = dot(first.astype(BF16), wzr_s[0:chans])
    for n, group in enumerate(groups[:-1]):
        for handle in relays[group[3][0][1]]:
            arrive(handle)
        mot_edges[n] = correlate(group)
    for copy in late:
        copy.wait()

    def shifted_sum(acc):
        line_no = lax.rem(
            lax.broadcasted_iota(jnp.int32, (acc.shape[0], chans), 0), width
        )
        before = pltpu.roll(acc[:, 0:chans], 1, 0)
        after = pltpu.roll(acc[:, 2 * chans : 3 * chans], acc.shape[0] - 1, 0)
        return (
            jnp.where(line_no > 0, before, 0.0)
            + acc[:, chans : 2 * chans]
            + jnp.where(line_no < width - 1, after, 0.0)
        )

    def recur(k, group):
        _, _, start, members = group
        n = len(members)
        for m, (i, _) in enumerate(members):
            c = start + m
            state = st[k, i].reshape(tall, chans).astype(F32)
            xin = (mot[c].reshape(tall, chans).astype(F32) + state).astype(BF16)
            known = hw0[i] if k == 0 else hw[c]
            gates = dot(xin, wzr_s[chans : 2 * chans]) + known
            zbuf[c] = jax.nn.sigmoid(gates[width : width + rows, 0:chans])
            reset = jax.nn.sigmoid(gates[:, chans : 2 * chans])
            if k == 0:
                h = th[i]
            else:
                h = jnp.concatenate(
                    [
                        hh[k - 1, c, 0].astype(F32), hid[c],
                        hh[k - 1, c, height + 1].astype(F32),
                    ],
                    axis=0,
                )
            qbuf[c, :, :, 0:chans] = (reset * h).astype(BF16).reshape(height + 2, width, chans)
            qbuf[c, :, :, chans : 2 * chans] = xin.reshape(height + 2, width, chans)
        taps = [
            qbuf[start : start + n, t : t + height].reshape(n * rows, 2 * chans) for t in range(3)
        ]
        total = shifted_sum(dot(jnp.concatenate(taps, axis=1), wq_s[...]))
        for m, (i, j) in enumerate(members):
            c = start + m
            h = th[i, width : width + rows] if k == 0 else hid[c]
            z = zbuf[c]
            h = (1.0 - z) * h + z * jnp.tanh(total[m * rows : (m + 1) * rows])
            hid[c] = h
            if k < ROUNDS - 1:
                hh[k, c, 1 : height + 1] = h.astype(BF16).reshape(height, width, chans)
        if k < ROUNDS - 1:
            span = pl.ds(start, n)
            return [
                push(side, hh.at[k, span, line_src[side]], hh.at[k, span, line_dst[side]])
                for side in (UP, DOWN)
            ]
        return []

    def gather(members, start, pick):
        chosen = [start + m for m, member in enumerate(members) if pick(*member)]
        total = None
        for c in chosen:
            term = times(c) * hid[c]
            total = term if total is None else total + term
        return total

    hid_edges = {}
    for k in range(ROUNDS):
        parcels = []
        for n, group in enumerate(groups):
            way, j, start, members = group
            if k == 0:
                for handle in mot_edges[n]:
                    arrive(handle)
            hid_edges[n] = recur(k, group)
            if way is not None:
                tosend = gather(members, start, lambda i, t: True).astype(BF16)
                msend[k, way, j] = dot(tosend, wmsg_s[chans : 2 * chans]).astype(BF16)
                parcels.append(push(way, msend.at[k, way, j], mrecv.at[k, way, j]))
        everything = [(c, m) for g in groups for c, m in enumerate(g[3], g[2])]
        for i in range(fd):
            first_sum = None
            second_sum = jnp.zeros((rows, chans), F32)
            for c, (s, t) in everything:
                if s == i:
                    term = times(c) * hid[c]
                    first_sum = term if first_sum is None else first_sum + term
                if t == fd + i:
                    second_sum = second_sum + times(c) * hid[c]
            pieces = jnp.concatenate([first_sum.astype(BF16), second_sum.astype(BF16)], axis=1)
            mown[i] = dot(pieces, wmsg_s[...])

        def ahead(n):
            _, _, start, members = groups[n]
            for handle in hid_edges[n]:
                arrive(handle)
            for m in range(len(members)):
                c = start + m
                hw[c] = dot(hh[k, c].reshape(tall, chans), wzr_s[0:chans])

        if k < ROUNDS - 1:
            for n in range(len(groups) - 1):
                ahead(n)
        for handle in parcels:
            arrive(handle)
        for i in range(fd):
            total = mown[i] + mrecv[k, LEFT, i].astype(F32) + mrecv[k, RIGHT, i].astype(F32)
            ubuf[k, i, 2 : height + 2] = (
                jnp.maximum(total, 0.0).astype(BF16).reshape(height, width, chans)
            )
        reach = 2 if k < ROUNDS - 1 else 1
        u_src = {UP: pl.ds(2, reach), DOWN: pl.ds(height + 2 - reach, reach)}
        u_dst = {UP: pl.ds(height + 2, reach), DOWN: pl.ds(2 - reach, reach)}
        u_edges = [
            push(side, ubuf.at[k, :, u_src[side]], ubuf.at[k, :, u_dst[side]])
            for side in (UP, DOWN)
        ]
        if k < ROUNDS - 1:
            ahead(len(groups) - 1)
        for handle in u_edges:
            arrive(handle)
        lines = height + 2 * (reach - 1)
        for i in range(fd):
            taps = [
                ubuf[k, i, 2 - reach + t : 2 - reach + t + lines].reshape(lines * width, chans)
                for t in range(3)
            ]
            moved = shifted_sum(dot(jnp.concatenate(taps, axis=1), wres_s[...]))
            old = st[k, i, 2 - reach : 2 - reach + lines] if k < ROUNDS - 1 else st[k, i, 1 : height + 1]
            new = (old.reshape(lines * width, chans).astype(F32) + moved).astype(BF16)
            new = new.reshape(lines, width, chans)
            if k == ROUNDS - 1:
                out_ref[i] = new
            else:
                st[k + 1, i] = new
        if k < ROUNDS - 1:
            for way, edge in ((UP, r == 0), (DOWN, r == nr - 1)):
                @pl.when(edge)
                def _(way=way):
                    st[k + 1, :, line_dst[back[way]]] = jnp.zeros((fd, width, chans), BF16)

    for handle in sent:
        @pl.when(both(has[handle[1]], handle[4]))
        def _(handle=handle):
            rcopy(handle).wait_send()


def local(nf, nr, fmap, context, pairs, w_corr, w_zr, w_q, w_msg, w_res):
    fd, height, width, chans = fmap.shape
    rows = height * width
    tall = rows + 2 * width
    win = 3 * fd
    groups, combos = plan(fd)
    tiles = -(-SPAN // (LANES // width))
    copies = 2 * fd + 2 + 2 + 4 * fd + 2 * len(groups) * ROUNDS + ROUNDS * (2 * fd + 2)
    hbm = pl.BlockSpec(memory_space=pl.ANY)
    return pl.pallas_call(
        functools.partial(kernel, nf, nr),
        out_shape=jax.ShapeDtypeStruct(fmap.shape, BF16),
        in_specs=[pl.BlockSpec(memory_space=pltpu.SMEM)] + [hbm] * 7,
        out_specs=pl.BlockSpec(memory_space=pltpu.VMEM),
        scratch_shapes=[
            pltpu.VMEM((height, fd, width, chans), BF16),
            pltpu.VMEM((win, 2 * RADIUS + height + 1, width, chans), BF16),
            pltpu.VMEM((ROUNDS, fd, height + 2, width, chans), BF16),
            pltpu.VMEM((combos, height + 2, width, chans), BF16),
            pltpu.VMEM((combos, rows, chans), F32),
            pltpu.VMEM((ROUNDS - 1, combos, height + 2, width, chans), BF16),
            pltpu.VMEM((fd, tall, chans), F32),
            pltpu.VMEM((fd, tall, 2 * chans), F32),
            pltpu.VMEM((combos, tall, 2 * chans), F32),
            pltpu.VMEM((combos, height + 2, width, 2 * chans), BF16),
            pltpu.VMEM((combos, rows, chans), F32),
            pltpu.VMEM((fd, rows, chans), F32),
            pltpu.VMEM((fd, rows, chans), F32),
            pltpu.VMEM((ROUNDS, 2, fd, rows, chans), BF16),
            pltpu.VMEM((ROUNDS, 2, fd, rows, chans), BF16),
            pltpu.VMEM((ROUNDS, fd, height + 4, width, chans), BF16),
            pltpu.VMEM((fd, rows, chans), F32),
            pltpu.VMEM(w_corr.shape, BF16),
            pltpu.VMEM((tiles * LANES, chans), BF16),
            pltpu.VMEM(w_zr.shape, BF16),
            pltpu.VMEM((6 * chans, 3 * chans), BF16),
            pltpu.VMEM((3 * chans, 3 * chans), BF16),
            pltpu.VMEM((2 * chans, chans), BF16),
            pltpu.SMEM((combos,), jnp.int32),
            pltpu.SemaphoreType.DMA((copies,)),
            pltpu.SemaphoreType.DMA((copies,)),
            pltpu.SemaphoreType.DMA((fd + 23,)),
        ],
        compiler_params=pltpu.CompilerParams(collective_id=0, has_side_effects=True),
    )(pairs.T, fmap, context, w_corr, w_zr, w_q, w_msg, w_res)


def solution(mesh):
    placed = (P("frames", "rows", None, None), P("frames", "rows", None, None)) + (P(),) * 6
    return jax.shard_map(
        functools.partial(local, mesh.shape["frames"], mesh.shape["rows"]),
        mesh=mesh,
        in_specs=placed,
        out_specs=P("frames", "rows", None, None),
        check_vma=False,
    )
```

```python
import functools

import jax
import jax.numpy as jnp
from jax import lax
from jax.experimental import pallas as pl
from jax.experimental.pallas import tpu as pltpu
from jax.sharding import PartitionSpec as P

RADIUS = 3
ROUNDS = 2
LANES = 128
SPAN = 2 * RADIUS + 1
MESH = pl.DeviceIdType.MESH
F32 = jnp.float32
BF16 = jnp.bfloat16
FAR, NEAR, UP, DOWN = range(4)


def dot(a, b):
    return jnp.dot(a, b, preferred_element_type=F32)


def dot_nt(a, b):
    return lax.dot_general(a, b, (((1,), (1,)), ((), ())), preferred_element_type=F32)


def plan(fd):
    groups = []
    for j in range(fd):
        for way, seat in ((FAR, j), (NEAR, 2 * fd + j)):
            groups.append((way, j, [(i, seat) for i in range(fd)]))
    groups.append((None, 0, [(i, fd + j) for j in range(fd) for i in range(fd) if i != j]))
    start = 0
    out = []
    for way, j, members in groups:
        out.append((way, j, start, members))
        start += len(members)
    return out, start


def kernel(
    nf, nr,
    pairs_ref, fmap_ref, ctx_ref, wcorr_ref, wzr_ref, wq_ref, wmsg_ref, wres_ref,
    out_ref,
    fsrc, fwin, st, mot, hid, hh, th, hw0, hw, qbuf, zbuf, asum, bsum,
    msend, mrecv, ubuf, mown,
    pairs_s, wcorr_s, wsel, wzr_s, wq_s, wres_s, wmsg_s, tbl,
    ssem, rsem, lsem,
):
    f = lax.axis_index("frames")
    r = lax.axis_index("rows")
    height, fd, width, chans = fsrc.shape
    npair = pairs_ref.shape[1]
    rows = height * width
    tall = (height + 2) * width
    groups, total_combos = plan(fd)
    step = 1 - 2 * lax.rem(f, 2)
    near, far = f + step, f - step
    has = {
        FAR: jnp.logical_and(far >= 0, far < nf), NEAR: jnp.logical_and(near >= 0, near < nf),
        UP: r > 0, DOWN: r < nr - 1,
    }
    dev = {FAR: (far, r), NEAR: (near, r), UP: (f, r - 1), DOWN: (f, r + 1)}
    back = {FAR: FAR, NEAR: NEAR, UP: DOWN, DOWN: UP}
    sent = []

    def both(cond, gate):
        return cond if gate is None else jnp.logical_and(cond, gate)

    def rcopy(handle):
        i, way, src, dst, _ = handle
        return pltpu.make_async_remote_copy(
            src_ref=src, dst_ref=dst, send_sem=ssem.at[i], recv_sem=rsem.at[i],
            device_id=dev[way], device_id_type=MESH,
        )

    def push(way, src, dst, gate=None):
        handle = (len(sent), way, src, dst, gate)
        sent.append(handle)

        @pl.when(both(has[way], gate))
        def _():
            rcopy(handle).start()

        return handle

    def arrive(handle):
        @pl.when(both(has[back[handle[1]]], handle[4]))
        def _():
            rcopy(handle).wait_recv()

    own_rows = pl.ds(RADIUS, height)
    middle = pl.ds(fd, fd)
    seat = {FAR: 0, NEAR: 2 * fd}

    barrier = pltpu.get_barrier_semaphore()
    count = 0
    for way in (FAR, NEAR, UP, DOWN):
        count = count + has[way].astype(jnp.int32)

        @pl.when(has[way])
        def _(way=way):
            pl.semaphore_signal(barrier, inc=1, device_id=dev[way], device_id_type=MESH)

    loads = []

    def load(src, dst):
        copy = pltpu.make_async_copy(src, dst, lsem.at[len(loads)])
        loads.append(copy)
        copy.start()
        return copy

    own_f = [load(fmap_ref.at[i], fsrc.at[:, i]) for i in range(fd)]
    own_c = load(ctx_ref, st.at[0, :, pl.ds(1, height)])
    listed = load(pairs_ref, pairs_s)
    corr_w = load(wcorr_ref, wcorr_s)
    gate_w = load(wzr_ref, wzr_s)
    late = []
    for k in range(3):
        for j in range(3):
            lanes = pl.ds(j * chans, chans)
            late.append(load(wq_ref.at[3 * k + j], wq_s.at[pl.ds(2 * k * chans, 2 * chans), lanes]))
            late.append(load(wres_ref.at[3 * k + j], wres_s.at[pl.ds(k * chans, chans), lanes]))
    for k in range(2):
        lanes = pl.ds(k * chans, chans)
        late.append(load(wmsg_ref.at[:, lanes], wmsg_s.at[lanes]))

    flip = jnp.where(
        lax.broadcasted_iota(jnp.int32, (width, width), 0)
        + lax.broadcasted_iota(jnp.int32, (width, width), 1)
        == width - 1,
        1.0,
        0.0,
    ).astype(BF16)
    for copy in own_f:
        copy.wait()
    for i in range(fd):
        for y in range(height):
            fwin[fd + i, RADIUS + y] = dot(flip, fsrc[y, i]).astype(BF16)
    pl.semaphore_wait(barrier, count)

    feats = {}
    edge_src = {UP: pl.ds(RADIUS, RADIUS), DOWN: pl.ds(height, RADIUS)}
    edge_dst = {UP: pl.ds(RADIUS + height, RADIUS), DOWN: pl.ds(0, RADIUS)}
    own_edges = [
        push(way, fwin.at[middle, edge_src[way]], fwin.at[middle, edge_dst[way]])
        for way in (UP, DOWN)
    ]
    for j in range(fd):
        for way in (FAR, NEAR):
            feats[way, j] = push(
                way, fwin.at[fd + j, own_rows], fwin.at[seat[way] + j, own_rows]
            )
    line_src = {UP: 1, DOWN: height}
    line_dst = {UP: height + 1, DOWN: 0}
    own_c.wait()
    ctx_edges = [
        push(way, st.at[0, :, line_src[way]], st.at[0, :, line_dst[way]]) for way in (UP, DOWN)
    ]

    fwin[:, 2 * RADIUS + height] = jnp.zeros((fwin.shape[0],) + fwin.shape[2:], BF16)
    for way, edge in ((UP, r == 0), (DOWN, r == nr - 1)):
        @pl.when(edge)
        def _(way=way):
            outside = back[way]
            fwin[:, edge_dst[outside]] = jnp.zeros(
                (fwin.shape[0], RADIUS, width, chans), BF16
            )
            line = line_dst[outside]
            mot[:, line] = jnp.zeros((total_combos, width, chans), BF16)
            hh[:, :, line] = jnp.zeros(hh.shape[:2] + (width, chans), BF16)
            st[0, :, line] = jnp.zeros((fd, width, chans), BF16)
            first = 0 if way == UP else height + 2
            ubuf[:, :, first : first + 2] = jnp.zeros((ROUNDS, fd, 2, width, chans), BF16)

    for way in (FAR, NEAR):
        @pl.when(jnp.logical_not(has[way]))
        def _(way=way):
            fwin[seat[way] : seat[way] + fd] = jnp.zeros((fd,) + fwin.shape[1:], BF16)
            for k in range(ROUNDS):
                mrecv[k, way] = jnp.zeros((fd, rows, chans), BF16)

    window = 3 * fd
    bases = [base * fd for base in (far, f, near)]
    codes = [i * window + j for _, _, _, members in groups for i, j in members]

    def tally(p, counts):
        i = pairs_s[0, p] - bases[1]
        own = jnp.logical_and(i >= 0, i < fd)
        code = jnp.int32(-1)
        for n, base in enumerate(bases):
            j = pairs_s[1, p] - base
            here = jnp.logical_and(own, jnp.logical_and(j >= 0, j < fd))
            code = jnp.where(here, i * window + n * fd + j, code)
        return tuple(v + (code == c).astype(jnp.int32) for v, c in zip(counts, codes))

    listed.wait()
    counts = lax.fori_loop(0, npair, tally, (jnp.int32(0),) * total_combos)
    for c in range(total_combos):
        tbl[c] = counts[c]

    def times(c):
        return tbl[c].astype(F32)

    per = LANES // width
    tiles = (SPAN + per - 1) // per
    depth = tiles * LANES
    origin = width - 1 - RADIUS

    def place(lane):
        spot = lax.rem(lane + (LANES - origin), LANES)
        return lax.div(spot, width), (SPAN - 1) - lax.rem(spot, width)

    corr_w.wait()
    line = lax.broadcasted_iota(jnp.int32, (depth, wcorr_s.shape[0]), 0)
    col = lax.broadcasted_iota(jnp.int32, (depth, wcorr_s.shape[0]), 1)
    half, b_off = place(lax.rem(line, LANES))
    a_off = lax.div(line, LANES) * per + half
    take = jnp.logical_and(b_off >= 0, a_off < SPAN)
    index = jnp.where(take, a_off * SPAN + b_off, -1)
    wsel[...] = dot(jnp.where(index == col, 1.0, 0.0).astype(BF16), wcorr_s[...]).astype(BF16)

    xs = lax.broadcasted_iota(jnp.int32, (width, LANES), 0)
    _, bs = place(lax.broadcasted_iota(jnp.int32, (width, LANES), 1))
    inside = jnp.logical_and(xs + bs >= RADIUS, xs + bs < width + RADIUS)
    inside = jnp.logical_and(inside, bs >= 0)
    scale = 1.0 / chans**0.5

    def banded(g):
        pieces = []
        for q in range(tiles):
            piece = pltpu.roll(g[:, q * LANES : (q + 1) * LANES], 0, 1, stride=1, stride_axis=0)
            pieces.append(jnp.where(inside, piece, 0.0).astype(BF16))
        return jnp.concatenate(pieces, axis=1)

    def correlate(group):
        way, _, start, members = group
        lines = [[] for _ in members]
        for y in range(height):
            if way is None:
                for n, (i, j) in enumerate(members):
                    b = fwin[j, y : y + tiles * per].reshape(tiles * per * width, chans)
                    lines[n].append(banded(dot_nt(fsrc[y, i], b)))
            else:
                j = members[0][1]
                b = fwin[j, y : y + tiles * per].reshape(tiles * per * width, chans)
                g = dot_nt(fsrc[y].reshape(fd * width, chans), b)
                for n in range(fd):
                    lines[n].append(banded(g[n * width : (n + 1) * width]))
        corr = jnp.concatenate([part for each in lines for part in each], axis=0)
        moved = jnp.maximum(dot(corr, wsel[...]) * scale, 0.0).astype(BF16)
        n = len(members)
        mot[start : start + n, 1 : height + 1] = moved.reshape(n, height, width, chans)
        span = pl.ds(start, n)
        return [
            push(side, mot.at[span, line_src[side]], mot.at[span, line_dst[side]])
            for side in (UP, DOWN)
        ]

    relays = {}

    def relay(j):
        for way in (FAR, NEAR):
            arrive(feats[way, j])
            spot = seat[way] + j
            relays[spot] = [
                push(
                    side, fwin.at[spot, edge_src[side]], fwin.at[spot, edge_dst[side]],
                    gate=has[back[way]],
                )
                for side in (UP, DOWN)
            ]

    relay(0)
    for handle in own_edges:
        arrive(handle)
    mot_edges = {len(groups) - 1: correlate(groups[-1])}
    for j in range(1, fd):
        relay(j)
    for handle in ctx_edges:
        arrive(handle)
    gate_w.wait()
    for i in range(fd):
        first = jnp.tanh(st[0, i].reshape(tall, chans).astype(F32))
        th[i] = first
        hw0[i] = dot(first.astype(BF16), wzr_s[0:chans])

    def compare(n):
        for handle in relays[groups[n][3][0][1]]:
            arrive(handle)
        mot_edges[n] = correlate(groups[n])

    remote = len(groups) - 1
    early = min(4, remote)
    for n in range(early):
        compare(n)
    for copy in late:
        copy.wait()

    def shifted_sum(acc):
        line_no = lax.rem(
            lax.broadcasted_iota(jnp.int32, (acc.shape[0], chans), 0), width
        )
        before = pltpu.roll(acc[:, 0:chans], 1, 0)
        after = pltpu.roll(acc[:, 2 * chans : 3 * chans], acc.shape[0] - 1, 0)
        return (
            jnp.where(line_no > 0, before, 0.0)
            + acc[:, chans : 2 * chans]
            + jnp.where(line_no < width - 1, after, 0.0)
        )

    def recur(k, group):
        _, _, start, members = group
        n = len(members)
        for m, (i, _) in enumerate(members):
            c = start + m
            state = st[k, i].reshape(tall, chans).astype(F32)
            xin = (mot[c].reshape(tall, chans).astype(F32) + state).astype(BF16)
            known = hw0[i] if k == 0 else hw[c]
            gates = dot(xin, wzr_s[chans : 2 * chans]) + known
            zbuf[c] = jax.nn.sigmoid(gates[width : width + rows, 0:chans])
            reset = jax.nn.sigmoid(gates[:, chans : 2 * chans])
            if k == 0:
                h = th[i]
            else:
                h = jnp.concatenate(
                    [
                        hh[k - 1, c, 0].astype(F32), hid[c],
                        hh[k - 1, c, height + 1].astype(F32),
                    ],
                    axis=0,
                )
            qbuf[c, :, :, 0:chans] = (reset * h).astype(BF16).reshape(height + 2, width, chans)
            qbuf[c, :, :, chans : 2 * chans] = xin.reshape(height + 2, width, chans)
        taps = [
            qbuf[start : start + n, t : t + height].reshape(n * rows, 2 * chans) for t in range(3)
        ]
        total = shifted_sum(dot(jnp.concatenate(taps, axis=1), wq_s[...]))
        for m, (i, j) in enumerate(members):
            c = start + m
            h = th[i, width : width + rows] if k == 0 else hid[c]
            z = zbuf[c]
            h = (1.0 - z) * h + z * jnp.tanh(total[m * rows : (m + 1) * rows])
            hid[c] = h
            if k < ROUNDS - 1:
                hh[k, c, 1 : height + 1] = h.astype(BF16).reshape(height, width, chans)
        if k < ROUNDS - 1:
            span = pl.ds(start, n)
            return [
                push(side, hh.at[k, span, line_src[side]], hh.at[k, span, line_dst[side]])
                for side in (UP, DOWN)
            ]
        return []

    def gather(members, start, pick):
        chosen = [start + m for m, member in enumerate(members) if pick(*member)]
        total = None
        for c in chosen:
            term = times(c) * hid[c]
            total = term if total is None else total + term
        return total

    hid_edges = {}
    for k in range(ROUNDS):
        parcels = {}
        for n, group in enumerate(groups):
            way, j, start, members = group
            if k == 0:
                if 0 < n <= remote - early:
                    compare(n + early - 1)
                for handle in mot_edges[n]:
                    arrive(handle)
            hid_edges[n] = recur(k, group)
            if way is not None:
                tosend = gather(members, start, lambda i, t: True).astype(BF16)
                msend[k, way, j] = dot(tosend, wmsg_s[chans : 2 * chans]).astype(BF16)
                parcels[way, j] = push(way, msend.at[k, way, j], mrecv.at[k, way, j])
        everything = [(c, m) for g in groups for c, m in enumerate(g[3], g[2])]
        for i in range(fd):
            first_sum = None
            second_sum = jnp.zeros((rows, chans), F32)
            for c, (s, t) in everything:
                if s == i:
                    term = times(c) * hid[c]
                    first_sum = term if first_sum is None else first_sum + term
                if t == fd + i:
                    second_sum = second_sum + times(c) * hid[c]
            pieces = jnp.concatenate([first_sum.astype(BF16), second_sum.astype(BF16)], axis=1)
            mown[i] = dot(pieces, wmsg_s[...])

        def ahead(n):
            _, _, start, members = groups[n]
            for handle in hid_edges[n]:
                arrive(handle)
            for m in range(len(members)):
                c = start + m
                hw[c] = dot(hh[k, c].reshape(tall, chans), wzr_s[0:chans])

        if k < ROUNDS - 1:
            for n in range(len(groups) - 1):
                ahead(n)
        reach = 2 if k < ROUNDS - 1 else 1
        u_src = {UP: pl.ds(2, reach), DOWN: pl.ds(height + 2 - reach, reach)}
        u_dst = {UP: pl.ds(height + 2, reach), DOWN: pl.ds(2 - reach, reach)}
        u_edges = []
        for i in range(fd):
            for way in (FAR, NEAR):
                arrive(parcels[way, i])
            total = mown[i] + mrecv[k, FAR, i].astype(F32) + mrecv[k, NEAR, i].astype(F32)
            ubuf[k, i, 2 : height + 2] = (
                jnp.maximum(total, 0.0).astype(BF16).reshape(height, width, chans)
            )
            u_edges.append([
                push(side, ubuf.at[k, i, u_src[side]], ubuf.at[k, i, u_dst[side]])
                for side in (UP, DOWN)
            ])
        if k < ROUNDS - 1:
            ahead(len(groups) - 1)
        lines = height + 2 * (reach - 1)
        for i in range(fd):
            for handle in u_edges[i]:
                arrive(handle)
            taps = [
                ubuf[k, i, 2 - reach + t : 2 - reach + t + lines].reshape(lines * width, chans)
                for t in range(3)
            ]
            moved = shifted_sum(dot(jnp.concatenate(taps, axis=1), wres_s[...]))
            first = 2 - reach if k < ROUNDS - 1 else 1
            old = st[k, i, first : first + lines].reshape(lines * width, chans)
            new = (old.astype(F32) + moved).astype(BF16).reshape(lines, width, chans)
            if k == ROUNDS - 1:
                out_ref[i] = new
            else:
                st[k + 1, i] = new
        if k < ROUNDS - 1:
            for way, edge in ((UP, r == 0), (DOWN, r == nr - 1)):
                @pl.when(edge)
                def _(way=way):
                    st[k + 1, :, line_dst[back[way]]] = jnp.zeros((fd, width, chans), BF16)

    for handle in sent:
        @pl.when(both(has[handle[1]], handle[4]))
        def _(handle=handle):
            rcopy(handle).wait_send()


def local(nf, nr, fmap, context, pairs, w_corr, w_zr, w_q, w_msg, w_res):
    fd, height, width, chans = fmap.shape
    rows = height * width
    tall = rows + 2 * width
    win = 3 * fd
    groups, combos = plan(fd)
    tiles = -(-SPAN // (LANES // width))
    copies = 2 * fd + 2 + 2 + 4 * fd + 2 * len(groups) * ROUNDS + ROUNDS * 4 * fd
    hbm = pl.BlockSpec(memory_space=pl.ANY)
    return pl.pallas_call(
        functools.partial(kernel, nf, nr),
        out_shape=pltpu.VMEM(fmap.shape, BF16),
        in_specs=[hbm] * 8,
        out_specs=pl.BlockSpec(memory_space=pltpu.VMEM),
        scratch_shapes=[
            pltpu.VMEM((height, fd, width, chans), BF16),
            pltpu.VMEM((win, 2 * RADIUS + height + 1, width, chans), BF16),
            pltpu.VMEM((ROUNDS, fd, height + 2, width, chans), BF16),
            pltpu.VMEM((combos, height + 2, width, chans), BF16),
            pltpu.VMEM((combos, rows, chans), F32),
            pltpu.VMEM((ROUNDS - 1, combos, height + 2, width, chans), BF16),
            pltpu.VMEM((fd, tall, chans), F32),
            pltpu.VMEM((fd, tall, 2 * chans), F32),
            pltpu.VMEM((combos, tall, 2 * chans), F32),
            pltpu.VMEM((combos, height + 2, width, 2 * chans), BF16),
            pltpu.VMEM((combos, rows, chans), F32),
            pltpu.VMEM((fd, rows, chans), F32),
            pltpu.VMEM((fd, rows, chans), F32),
            pltpu.VMEM((ROUNDS, 2, fd, rows, chans), BF16),
            pltpu.VMEM((ROUNDS, 2, fd, rows, chans), BF16),
            pltpu.VMEM((ROUNDS, fd, height + 4, width, chans), BF16),
            pltpu.VMEM((fd, rows, chans), F32),
            pltpu.SMEM((3, pairs.shape[0]), jnp.int32),
            pltpu.VMEM(w_corr.shape, BF16),
            pltpu.VMEM((tiles * LANES, chans), BF16),
            pltpu.VMEM(w_zr.shape, BF16),
            pltpu.VMEM((6 * chans, 3 * chans), BF16),
            pltpu.VMEM((3 * chans, 3 * chans), BF16),
            pltpu.VMEM((2 * chans, chans), BF16),
            pltpu.SMEM((combos,), jnp.int32),
            pltpu.SemaphoreType.DMA((copies,)),
            pltpu.SemaphoreType.DMA((copies,)),
            pltpu.SemaphoreType.DMA((fd + 24,)),
        ],
        compiler_params=pltpu.CompilerParams(collective_id=0, has_side_effects=True),
    )(pairs.T, fmap, context, w_corr, w_zr, w_q, w_msg, w_res)


def solution(mesh):
    placed = (P("frames", "rows", None, None), P("frames", "rows", None, None)) + (P(),) * 6
    return jax.shard_map(
        functools.partial(local, mesh.shape["frames"], mesh.shape["rows"]),
        mesh=mesh,
        in_specs=placed,
        out_specs=P("frames", "rows", None, None),
        check_vma=False,
    )
```

```python
import functools
import math

import jax
import jax.numpy as jnp
from jax import lax
from jax.experimental import pallas as pl
from jax.experimental.pallas import tpu as pltpu
from jax.sharding import PartitionSpec as P

RADIUS = 3
ROUNDS = 2
LATE = True
LANES = 128
SPAN = 2 * RADIUS + 1
MESH = pl.DeviceIdType.MESH
F32 = jnp.float32
BF16 = jnp.bfloat16
FAR, NEAR, UP, DOWN = range(4)


def dot(a, b):
    return jnp.dot(a, b, preferred_element_type=F32)


def dot_nt(a, b):
    return lax.dot_general(a, b, (((1,), (1,)), ((), ())), preferred_element_type=F32)


def plan(fd):
    groups = []
    for j in range(fd):
        for way, seat in ((FAR, j), (NEAR, 2 * fd + j)):
            groups.append((way, j, [(i, seat) for i in range(fd)]))
    groups.append((None, 0, [(i, fd + j) for j in range(fd) for i in range(fd) if i != j]))
    start = 0
    out = []
    for way, j, members in groups:
        out.append((way, j, start, members))
        start += len(members)
    return out, start


def kernel(
    nf, nr,
    pairs_ref, fmap_ref, ctx_ref, wcorr_ref, wzr_ref, wq_ref, wmsg_ref, wres_ref,
    out_ref,
    fsrc, fwin, st, mot, hid, hh, th, hw0, hw, qbuf, zbuf,
    msend, mrecv, ubuf, mown, town,
    bulk, pairs_s, wcorr_s, wsel, wzr_s, wq_s, wres_s, wmsg_s, tbl,
    ssem, rsem, lsem,
):
    f = lax.axis_index("frames")
    r = lax.axis_index("rows")
    height, fd, width, chans = fsrc.shape
    npair = pairs_ref.shape[1]
    rows = height * width
    tall = (height + 2) * width
    groups, total_combos = plan(fd)
    step = 1 - 2 * lax.rem(f, 2)
    near, far = f + step, f - step
    has = {
        FAR: jnp.logical_and(far >= 0, far < nf), NEAR: jnp.logical_and(near >= 0, near < nf),
        UP: r > 0, DOWN: r < nr - 1,
    }
    dev = {FAR: (far, r), NEAR: (near, r), UP: (f, r - 1), DOWN: (f, r + 1)}
    back = {FAR: FAR, NEAR: NEAR, UP: DOWN, DOWN: UP}
    sent = {}
    landed = []

    def both(cond, gate):
        return cond if gate is None else jnp.logical_and(cond, gate)

    def rcopy(way, src, dst, send_sem, recv_sem):
        return pltpu.make_async_remote_copy(
            src_ref=src, dst_ref=dst, send_sem=send_sem, recv_sem=recv_sem,
            device_id=dev[way], device_id_type=MESH,
        )

    def lines_of(ref):
        return math.prod(ref.shape) // (width * chans)

    kinds = [(way, None) for way in (FAR, NEAR, UP, DOWN)]
    kinds += [(side, way) for side in (UP, DOWN) for way in (FAR, NEAR)]

    def push(copies, gate=None):
        spot = len(landed)
        landed.append(None)
        for way, src, dst in copies:
            kind = kinds.index((way, gate))
            sent[kind] = sent.get(kind, 0) + lines_of(src)

            @pl.when(both(has[way], None if gate is None else has[gate]))
            def _(way=way, src=src, dst=dst, kind=kind):
                rcopy(way, src, dst, ssem.at[kind], rsem.at[spot]).start()

        return spot, [way for way, _, _ in copies], lines_of(copies[0][1]), gate

    def await_lines(way, spot, lines):
        part = bulk.at[pl.ds(0, lines)]
        rcopy(way, part, part, ssem.at[0], rsem.at[spot]).wait_recv()

    def arrive(handle):
        spot, ways, lines, gate = handle
        gate = None if gate is None else has[gate]
        if len(ways) == 1:
            @pl.when(both(has[back[ways[0]]], gate))
            def _():
                await_lines(ways[0], spot, lines)
        else:
            here, there = (has[back[way]] for way in ways)

            @pl.when(both(jnp.logical_and(here, there), gate))
            def _():
                await_lines(ways[0], spot, 2 * lines)

            @pl.when(both(jnp.not_equal(here, there), gate))
            def _():
                await_lines(ways[0], spot, lines)

    own_rows = pl.ds(RADIUS, height)
    middle = pl.ds(fd, fd)
    seat = {FAR: 0, NEAR: 2 * fd}

    barrier = pltpu.get_barrier_semaphore()
    count = 0
    for way in (FAR, NEAR, UP, DOWN):
        count = count + has[way].astype(jnp.int32)

        @pl.when(has[way])
        def _(way=way):
            pl.semaphore_signal(barrier, inc=1, device_id=dev[way], device_id_type=MESH)

    class Load:
        def __init__(self, n, whole, copies):
            self.n, self.whole = n, whole
            for src, dst in copies:
                pltpu.make_async_copy(src, dst, lsem.at[n]).start()

        def wait(self):
            pltpu.make_async_copy(self.whole, self.whole, lsem.at[self.n]).wait()

    def lanes(j):
        return pl.ds(j * chans, chans)

    taps = [(k, j) for k in range(3) for j in range(3)]
    own_f = Load(0, fsrc, [(fmap_ref.at[i], fsrc.at[:, i]) for i in range(fd)])
    own_c = pltpu.make_async_copy(ctx_ref, st.at[0, :, pl.ds(1, height)], lsem.at[1])
    own_c.start()
    listed = Load(2, pairs_s, [(pairs_ref, pairs_s)])
    corr_w = Load(3, wcorr_s, [(wcorr_ref, wcorr_s)])
    gate_w = Load(4, wzr_s, [(wzr_ref, wzr_s)])
    late = [
        Load(5, wq_s, [
            (wq_ref.at[3 * k + j], wq_s.at[pl.ds(2 * k * chans, 2 * chans), lanes(j)])
            for k, j in taps
        ]),
        Load(6, wres_s, [
            (wres_ref.at[3 * k + j], wres_s.at[lanes(k), lanes(j)]) for k, j in taps
        ]),
        Load(7, wmsg_s, [(wmsg_ref.at[:, lanes(k)], wmsg_s.at[lanes(k)]) for k in range(2)]),
    ]

    flip = jnp.where(
        lax.broadcasted_iota(jnp.int32, (width, width), 0)
        + lax.broadcasted_iota(jnp.int32, (width, width), 1)
        == width - 1,
        1.0,
        0.0,
    ).astype(BF16)
    own_f.wait()
    for i in range(fd):
        for y in range(height):
            fwin[fd + i, RADIUS + y] = dot(flip, fsrc[y, i]).astype(BF16)
    pl.semaphore_wait(barrier, count)

    feats = {}
    edge_src = {UP: pl.ds(RADIUS, RADIUS), DOWN: pl.ds(height, RADIUS)}
    edge_dst = {UP: pl.ds(RADIUS + height, RADIUS), DOWN: pl.ds(0, RADIUS)}
    own_edges = push([
        (way, fwin.at[middle, edge_src[way]], fwin.at[middle, edge_dst[way]])
        for way in (UP, DOWN)
    ])

    def offer(j):
        for way in (FAR, NEAR):
            feats[way, j] = push([
                (way, fwin.at[fd + j, own_rows], fwin.at[seat[way] + j, own_rows])
            ])

    offer(0)
    line_src = {UP: 1, DOWN: height}
    line_dst = {UP: height + 1, DOWN: 0}
    own_c.wait()
    ctx_edges = push([
        (way, st.at[0, :, line_src[way]], st.at[0, :, line_dst[way]]) for way in (UP, DOWN)
    ])
    if not LATE:
        for j in range(1, fd):
            offer(j)

    fwin[:, 2 * RADIUS + height] = jnp.zeros((fwin.shape[0],) + fwin.shape[2:], BF16)
    for way, edge in ((UP, r == 0), (DOWN, r == nr - 1)):
        @pl.when(edge)
        def _(way=way):
            outside = back[way]
            fwin[:, edge_dst[outside]] = jnp.zeros(
                (fwin.shape[0], RADIUS, width, chans), BF16
            )
            line = line_dst[outside]
            mot[:, line] = jnp.zeros((total_combos, width, chans), BF16)
            hh[:, :, line] = jnp.zeros(hh.shape[:2] + (width, chans), BF16)
            st[0, :, line] = jnp.zeros((fd, width, chans), BF16)
            first = 0 if way == UP else height + 2
            ubuf[:, :, first : first + 2] = jnp.zeros((ROUNDS, fd, 2, width, chans), BF16)

    for way in (FAR, NEAR):
        @pl.when(jnp.logical_not(has[way]))
        def _(way=way):
            fwin[seat[way] : seat[way] + fd] = jnp.zeros((fd,) + fwin.shape[1:], BF16)
            for k in range(ROUNDS):
                mrecv[k, way] = jnp.zeros((fd, rows, chans), BF16)

    window = 3 * fd
    bases = [base * fd for base in (far, f, near)]
    codes = [i * window + j for _, _, _, members in groups for i, j in members]

    def tally(p, counts):
        i = pairs_s[0, p] - bases[1]
        own = jnp.logical_and(i >= 0, i < fd)
        code = jnp.int32(-1)
        for n, base in enumerate(bases):
            j = pairs_s[1, p] - base
            here = jnp.logical_and(own, jnp.logical_and(j >= 0, j < fd))
            code = jnp.where(here, i * window + n * fd + j, code)
        return tuple(v + (code == c).astype(jnp.int32) for v, c in zip(counts, codes))

    listed.wait()
    counts = lax.fori_loop(0, npair, tally, (jnp.int32(0),) * total_combos)
    for c in range(total_combos):
        tbl[c] = counts[c]

    def times(c):
        return tbl[c].astype(F32)

    per = LANES // width
    tiles = (SPAN + per - 1) // per
    depth = tiles * LANES
    origin = width - 1 - RADIUS

    def place(lane):
        spot = lax.rem(lane + (LANES - origin), LANES)
        return lax.div(spot, width), (SPAN - 1) - lax.rem(spot, width)

    corr_w.wait()
    line = lax.broadcasted_iota(jnp.int32, (depth, wcorr_s.shape[0]), 0)
    col = lax.broadcasted_iota(jnp.int32, (depth, wcorr_s.shape[0]), 1)
    half, b_off = place(lax.rem(line, LANES))
    a_off = lax.div(line, LANES) * per + half
    take = jnp.logical_and(b_off >= 0, a_off < SPAN)
    index = jnp.where(take, a_off * SPAN + b_off, -1)
    wsel[...] = dot(jnp.where(index == col, 1.0, 0.0).astype(BF16), wcorr_s[...]).astype(BF16)

    xs = lax.broadcasted_iota(jnp.int32, (width, LANES), 0)
    _, bs = place(lax.broadcasted_iota(jnp.int32, (width, LANES), 1))
    inside = jnp.logical_and(xs + bs >= RADIUS, xs + bs < width + RADIUS)
    inside = jnp.logical_and(inside, bs >= 0)
    scale = 1.0 / chans**0.5

    def banded(g):
        pieces = []
        for q in range(tiles):
            piece = pltpu.roll(g[:, q * LANES : (q + 1) * LANES], 0, 1, stride=1, stride_axis=0)
            pieces.append(jnp.where(inside, piece, 0.0).astype(BF16))
        return jnp.concatenate(pieces, axis=1)

    def correlate(group):
        way, _, start, members = group
        lines = [[] for _ in members]
        for y in range(height):
            if way is None:
                for n, (i, j) in enumerate(members):
                    b = fwin[j, y : y + tiles * per].reshape(tiles * per * width, chans)
                    lines[n].append(banded(dot_nt(fsrc[y, i], b)))
            else:
                j = members[0][1]
                b = fwin[j, y : y + tiles * per].reshape(tiles * per * width, chans)
                g = dot_nt(fsrc[y].reshape(fd * width, chans), b)
                for n in range(fd):
                    lines[n].append(banded(g[n * width : (n + 1) * width]))
        corr = jnp.concatenate([part for each in lines for part in each], axis=0)
        moved = jnp.maximum(dot(corr, wsel[...]) * scale, 0.0).astype(BF16)
        n = len(members)
        mot[start : start + n, 1 : height + 1] = moved.reshape(n, height, width, chans)
        span = pl.ds(start, n)
        return push([
            (side, mot.at[span, line_src[side]], mot.at[span, line_dst[side]])
            for side in (UP, DOWN)
        ])

    relays = {}
    if LATE:
        for j in range(1, fd):
            offer(j)

    def relay(j):
        for way in (FAR, NEAR):
            arrive(feats[way, j])
            spot = seat[way] + j
            relays[spot] = push(
                [
                    (side, fwin.at[spot, edge_src[side]], fwin.at[spot, edge_dst[side]])
                    for side in (UP, DOWN)
                ],
                gate=way,
            )

    relay(0)
    arrive(own_edges)
    mot_edges = {len(groups) - 1: correlate(groups[-1])}
    for j in range(1, fd):
        relay(j)
    arrive(ctx_edges)
    gate_w.wait()
    for i in range(fd):
        first = jnp.tanh(st[0, i].reshape(tall, chans).astype(F32))
        th[i] = first
        hw0[i] = dot(first.astype(BF16), wzr_s[0:chans])

    def compare(n):
        arrive(relays[groups[n][3][0][1]])
        mot_edges[n] = correlate(groups[n])

    remote = len(groups) - 1
    early = min(4, remote)
    for n in range(early):
        compare(n)
    for copy in late:
        copy.wait()

    def shifted_sum(acc):
        line_no = lax.rem(
            lax.broadcasted_iota(jnp.int32, (acc.shape[0], chans), 0), width
        )
        before = pltpu.roll(acc[:, 0:chans], 1, 0)
        after = pltpu.roll(acc[:, 2 * chans : 3 * chans], acc.shape[0] - 1, 0)
        return (
            jnp.where(line_no > 0, before, 0.0)
            + acc[:, chans : 2 * chans]
            + jnp.where(line_no < width - 1, after, 0.0)
        )

    gated = set()

    def gate(k, c, i):
        gated.add((k, c))
        state = st[k, i].reshape(tall, chans).astype(F32)
        xin = (mot[c].reshape(tall, chans).astype(F32) + state).astype(BF16)
        known = hw0[i] if k == 0 else hw[c]
        gates = dot(xin, wzr_s[chans : 2 * chans]) + known
        zbuf[c] = jax.nn.sigmoid(gates[width : width + rows, 0:chans])
        reset = jax.nn.sigmoid(gates[:, chans : 2 * chans])
        if k == 0:
            h = th[i]
        else:
            h = jnp.concatenate(
                [
                    hh[k - 1, c, 0].astype(F32), hid[c],
                    hh[k - 1, c, height + 1].astype(F32),
                ],
                axis=0,
            )
        qbuf[c, :, :, 0:chans] = (reset * h).astype(BF16).reshape(height + 2, width, chans)
        qbuf[c, :, :, chans : 2 * chans] = xin.reshape(height + 2, width, chans)

    def recur(k, group):
        _, _, start, members = group
        n = len(members)
        for m, (i, _) in enumerate(members):
            if (k, start + m) not in gated:
                gate(k, start + m, i)
        taps = [
            qbuf[start : start + n, t : t + height].reshape(n * rows, 2 * chans) for t in range(3)
        ]
        total = shifted_sum(dot(jnp.concatenate(taps, axis=1), wq_s[...]))
        for m, (i, j) in enumerate(members):
            c = start + m
            h = th[i, width : width + rows] if k == 0 else hid[c]
            z = zbuf[c]
            h = (1.0 - z) * h + z * jnp.tanh(total[m * rows : (m + 1) * rows])
            hid[c] = h
            if k < ROUNDS - 1:
                hh[k, c, 1 : height + 1] = h.astype(BF16).reshape(height, width, chans)
        if k < ROUNDS - 1:
            span = pl.ds(start, n)
            return push([
                (side, hh.at[k, span, line_src[side]], hh.at[k, span, line_dst[side]])
                for side in (UP, DOWN)
            ])
        return None

    def gather(members, start):
        total = None
        for c in range(start, start + len(members)):
            term = times(c) * hid[c]
            total = term if total is None else total + term
        return total

    hid_edges = {}
    for k in range(ROUNDS):
        parcels = {}
        for n, group in enumerate(groups):
            way, j, start, members = group
            if k == 0:
                if 0 < n <= remote - early:
                    compare(n + early - 1)
                arrive(mot_edges[n])
            hid_edges[n] = recur(k, group)
            if way is not None:
                msend[k, way, j] = gather(members, start).astype(BF16)
                parcels[way, j] = push([
                    (way, msend.at[k, way, j], mrecv.at[k, way, j])
                ])
        everything = [(c, m) for g in groups for c, m in enumerate(g[3], g[2])]
        for i in range(fd):
            first_sum = None
            second_sum = jnp.zeros((rows, chans), F32)
            for c, (s, t) in everything:
                if s == i:
                    term = times(c) * hid[c]
                    first_sum = term if first_sum is None else first_sum + term
                if t == fd + i:
                    second_sum = second_sum + times(c) * hid[c]
            mown[i] = dot(first_sum.astype(BF16), wmsg_s[0:chans])
            town[i] = second_sum

        def ahead(n):
            _, _, start, members = groups[n]
            arrive(hid_edges[n])
            for m in range(len(members)):
                c = start + m
                hw[c] = dot(hh[k, c].reshape(tall, chans), wzr_s[0:chans])

        reach = 2 if k < ROUNDS - 1 else 1
        lines = height + 2 * (reach - 1)
        u_src = {UP: pl.ds(2, reach), DOWN: pl.ds(height + 2 - reach, reach)}
        u_dst = {UP: pl.ds(height + 2, reach), DOWN: pl.ds(2 - reach, reach)}
        u_edges = {}

        def update(i):
            for way in (FAR, NEAR):
                arrive(parcels[way, i])
            arrived = mrecv[k, FAR, i].astype(F32) + mrecv[k, NEAR, i].astype(F32)
            second = (town[i] + arrived).astype(BF16)
            total = mown[i] + dot(second, wmsg_s[chans : 2 * chans])
            ubuf[k, i, 2 : height + 2] = (
                jnp.maximum(total, 0.0).astype(BF16).reshape(height, width, chans)
            )
            u_edges[i] = push([
                (side, ubuf.at[k, i, u_src[side]], ubuf.at[k, i, u_dst[side]])
                for side in (UP, DOWN)
            ])

        def inner(i):
            own = ubuf[k, i, 2 : height + 2].reshape(rows, chans)
            acc = dot(own, wres_s[chans : 2 * chans])
            blank = jnp.zeros((width, 3 * chans), F32)
            if height > 1:
                above = dot(own[: rows - width], wres_s[0:chans])
                below = dot(own[width:], wres_s[2 * chans : 3 * chans])
                acc = acc + jnp.concatenate([blank, above], axis=0)
                acc = acc + jnp.concatenate([below, blank], axis=0)
            old = st[k, i, 1 : height + 1].reshape(rows, chans)
            mown[i] = old.astype(F32) + shifted_sum(acc)

        def outer(i):
            arrive(u_edges[i])
            above = shifted_sum(dot(ubuf[k, i, 1], wres_s[0:chans]))
            below = shifted_sum(dot(ubuf[k, i, height + 2], wres_s[2 * chans : 3 * chans]))
            for y in range(height):
                total = mown[i, y * width : (y + 1) * width]
                if y == 0:
                    total = total + above
                if y == height - 1:
                    total = total + below
                out_ref[i, y] = total.astype(BF16)

        def residual(i):
            arrive(u_edges[i])
            taps = [
                ubuf[k, i, 2 - reach + t : 2 - reach + t + lines].reshape(lines * width, chans)
                for t in range(3)
            ]
            moved = shifted_sum(dot(jnp.concatenate(taps, axis=1), wres_s[...]))
            old = st[k, i].reshape(lines * width, chans)
            new = (old.astype(F32) + moved).astype(BF16).reshape(lines, width, chans)
            st[k + 1, i] = new
            for way, edge in ((UP, r == 0), (DOWN, r == nr - 1)):
                @pl.when(edge)
                def _(way=way):
                    st[k + 1, i, line_dst[back[way]]] = jnp.zeros((width, chans), BF16)

        fill = list(range(len(groups))) if k < ROUNDS - 1 else []
        for i in range(fd):
            update(i)
            for n in fill[: 2]:
                ahead(n)
            fill = fill[2:]
        if k == ROUNDS - 1:
            for i in range(fd):
                inner(i)
            for i in range(fd):
                outer(i)
        for i in range(fd if k < ROUNDS - 1 else 0):
            residual(i)
            if k < ROUNDS - 1:
                for n in fill:
                    ahead(n)
                fill = []
                if i < fd - 1:
                    for _, _, start, members in groups:
                        for m, (source, _) in enumerate(members):
                            if source == i:
                                gate(k + 1, start + m, source)

    for kind, lines in sorted(sent.items()):
        way, gate = kinds[kind]

        @pl.when(both(has[way], None if gate is None else has[gate]))
        def _(way=way, kind=kind, lines=lines):
            part = bulk.at[pl.ds(0, lines)]
            rcopy(way, part, part, ssem.at[kind], rsem.at[0]).wait_send()


def local(nf, nr, fmap, context, pairs, w_corr, w_zr, w_q, w_msg, w_res):
    fd, height, width, chans = fmap.shape
    rows = height * width
    tall = rows + 2 * width
    win = 3 * fd
    groups, combos = plan(fd)
    tiles = -(-SPAN // (LANES // width))
    copies = 4 * fd + 2 + len(groups) * ROUNDS + ROUNDS * 3 * fd
    hbm = pl.BlockSpec(memory_space=pl.ANY)
    return pl.pallas_call(
        functools.partial(kernel, nf, nr),
        out_shape=pltpu.VMEM(fmap.shape, BF16),
        in_specs=[hbm] * 8,
        out_specs=pl.BlockSpec(memory_space=pltpu.VMEM),
        scratch_shapes=[
            pltpu.VMEM((height, fd, width, chans), BF16),
            pltpu.VMEM((win, 2 * RADIUS + height + 1, width, chans), BF16),
            pltpu.VMEM((ROUNDS, fd, height + 2, width, chans), BF16),
            pltpu.VMEM((combos, height + 2, width, chans), BF16),
            pltpu.VMEM((combos, rows, chans), F32),
            pltpu.VMEM((ROUNDS - 1, combos, height + 2, width, chans), BF16),
            pltpu.VMEM((fd, tall, chans), F32),
            pltpu.VMEM((fd, tall, 2 * chans), F32),
            pltpu.VMEM((combos, tall, 2 * chans), F32),
            pltpu.VMEM((combos, height + 2, width, 2 * chans), BF16),
            pltpu.VMEM((combos, rows, chans), F32),
            pltpu.VMEM((ROUNDS, 2, fd, rows, chans), BF16),
            pltpu.VMEM((ROUNDS, 2, fd, rows, chans), BF16),
            pltpu.VMEM((ROUNDS, fd, height + 4, width, chans), BF16),
            pltpu.VMEM((fd, rows, chans), F32),
            pltpu.VMEM((fd, rows, chans), F32),
            pltpu.VMEM((ROUNDS * (combos + 2 * fd) + 4 * fd, width, chans), BF16),
            pltpu.SMEM((3, pairs.shape[0]), jnp.int32),
            pltpu.VMEM(w_corr.shape, BF16),
            pltpu.VMEM((tiles * LANES, chans), BF16),
            pltpu.VMEM(w_zr.shape, BF16),
            pltpu.VMEM((6 * chans, 3 * chans), BF16),
            pltpu.VMEM((3 * chans, 3 * chans), BF16),
            pltpu.VMEM((2 * chans, chans), BF16),
            pltpu.SMEM((combos,), jnp.int32),
            pltpu.SemaphoreType.DMA((8,)),
            pltpu.SemaphoreType.DMA((copies,)),
            pltpu.SemaphoreType.DMA((8,)),
        ],
        compiler_params=pltpu.CompilerParams(collective_id=0, has_side_effects=True),
    )(pairs.T, fmap, context, w_corr, w_zr, w_q, w_msg, w_res)


def solution(mesh):
    placed = (P("frames", "rows", None, None), P("frames", "rows", None, None)) + (P(),) * 6
    return jax.shard_map(
        functools.partial(local, mesh.shape["frames"], mesh.shape["rows"]),
        mesh=mesh,
        in_specs=placed,
        out_specs=P("frames", "rows", None, None),
        check_vma=False,
    )
```

```python
import functools
import math

import jax
import jax.numpy as jnp
from jax import lax
from jax.experimental import pallas as pl
from jax.experimental.pallas import tpu as pltpu
from jax.sharding import PartitionSpec as P

RADIUS = 3
ROUNDS = 2
LANES = 128
SPAN = 2 * RADIUS + 1
MESH = pl.DeviceIdType.MESH
F32 = jnp.float32
BF16 = jnp.bfloat16
FAR, NEAR, UP, DOWN = range(4)


def dot(a, b):
    return jnp.dot(a, b, preferred_element_type=F32)


def dot_nt(a, b):
    return lax.dot_general(a, b, (((1,), (1,)), ((), ())), preferred_element_type=F32)


def plan(fd):
    groups = []
    for j in range(fd):
        for way, seat in ((FAR, j), (NEAR, 2 * fd + j)):
            groups.append((way, j, [(i, seat) for i in range(fd)]))
    groups.append((None, 0, [(i, fd + j) for j in range(fd) for i in range(fd) if i != j]))
    start = 0
    out = []
    for way, j, members in groups:
        out.append((way, j, start, members))
        start += len(members)
    return out, start


def kernel(
    nf, nr,
    pairs_ref, fmap_ref, ctx_ref, wcorr_ref, wzr_ref, wq_ref, wmsg_ref, wres_ref,
    out_ref,
    fsrc, fwin, st, mot, hid, hh, th, hw0, hw, qbuf, zbuf,
    msend, mrecv, ubuf, mown, town,
    bulk, pairs_s, wcorr_s, wsel, wzr_s, wq_s, wres_s, wmsg_s, tbl,
    ssem, rsem, lsem,
):
    f = lax.axis_index("frames")
    r = lax.axis_index("rows")
    height, fd, width, chans = fsrc.shape
    npair = pairs_ref.shape[1]
    rows = height * width
    tall = (height + 2) * width
    groups, total_combos = plan(fd)
    step = 1 - 2 * lax.rem(f, 2)
    near, far = f + step, f - step
    has = {
        FAR: jnp.logical_and(far >= 0, far < nf), NEAR: jnp.logical_and(near >= 0, near < nf),
        UP: r > 0, DOWN: r < nr - 1,
    }
    dev = {FAR: (far, r), NEAR: (near, r), UP: (f, r - 1), DOWN: (f, r + 1)}
    back = {FAR: FAR, NEAR: NEAR, UP: DOWN, DOWN: UP}
    sent = {}
    landed = []

    def both(cond, gate):
        return cond if gate is None else jnp.logical_and(cond, gate)

    def rcopy(way, src, dst, send_sem, recv_sem):
        return pltpu.make_async_remote_copy(
            src_ref=src, dst_ref=dst, send_sem=send_sem, recv_sem=recv_sem,
            device_id=dev[way], device_id_type=MESH,
        )

    def lines_of(ref):
        return math.prod(ref.shape) // (width * chans)

    kinds = [(way, None) for way in (FAR, NEAR, UP, DOWN)]
    kinds += [(side, way) for side in (UP, DOWN) for way in (FAR, NEAR)]

    def push(copies, gate=None):
        spot = len(landed)
        landed.append(None)
        for way, src, dst in copies:
            kind = kinds.index((way, gate))
            sent[kind] = sent.get(kind, 0) + lines_of(src)

            @pl.when(both(has[way], None if gate is None else has[gate]))
            def _(way=way, src=src, dst=dst, kind=kind):
                rcopy(way, src, dst, ssem.at[kind], rsem.at[spot]).start()

        return spot, [way for way, _, _ in copies], lines_of(copies[0][1]), gate

    def await_lines(way, spot, lines):
        part = bulk.at[pl.ds(0, lines)]
        rcopy(way, part, part, ssem.at[0], rsem.at[spot]).wait_recv()

    def arrive(handle):
        spot, ways, lines, gate = handle
        gate = None if gate is None else has[gate]
        if len(ways) == 1:
            @pl.when(both(has[back[ways[0]]], gate))
            def _():
                await_lines(ways[0], spot, lines)
        else:
            here, there = (has[back[way]] for way in ways)

            @pl.when(both(jnp.logical_and(here, there), gate))
            def _():
                await_lines(ways[0], spot, 2 * lines)

            @pl.when(both(jnp.not_equal(here, there), gate))
            def _():
                await_lines(ways[0], spot, lines)

    own_rows = pl.ds(RADIUS, height)
    middle = pl.ds(fd, fd)
    seat = {FAR: 0, NEAR: 2 * fd}

    barrier = pltpu.get_barrier_semaphore()
    count = 0
    for way in (FAR, NEAR, UP, DOWN):
        count = count + has[way].astype(jnp.int32)

        @pl.when(has[way])
        def _(way=way):
            pl.semaphore_signal(barrier, inc=1, device_id=dev[way], device_id_type=MESH)

    class Load:
        def __init__(self, n, whole, copies):
            self.n, self.whole = n, whole
            for src, dst in copies:
                pltpu.make_async_copy(src, dst, lsem.at[n]).start()

        def wait(self):
            pltpu.make_async_copy(self.whole, self.whole, lsem.at[self.n]).wait()

    def lanes(j):
        return pl.ds(j * chans, chans)

    taps = [(k, j) for k in range(3) for j in range(3)]
    own_f = Load(0, fsrc, [(fmap_ref.at[i], fsrc.at[:, i]) for i in range(fd)])
    own_c = pltpu.make_async_copy(ctx_ref, st.at[0, :, pl.ds(1, height)], lsem.at[1])
    own_c.start()
    listed = Load(2, pairs_s, [(pairs_ref, pairs_s)])
    corr_w = Load(3, wcorr_s, [(wcorr_ref, wcorr_s)])
    gate_w = Load(4, wzr_s, [(wzr_ref, wzr_s)])
    late = [
        Load(5, wq_s, [
            (wq_ref.at[3 * k + j], wq_s.at[pl.ds(2 * k * chans, 2 * chans), lanes(j)])
            for k, j in taps
        ]),
        Load(6, wres_s, [
            (wres_ref.at[3 * k + j], wres_s.at[lanes(k), lanes(j)]) for k, j in taps
        ]),
        Load(7, wmsg_s, [(wmsg_ref.at[:, lanes(k)], wmsg_s.at[lanes(k)]) for k in range(2)]),
    ]

    flip = jnp.where(
        lax.broadcasted_iota(jnp.int32, (width, width), 0)
        + lax.broadcasted_iota(jnp.int32, (width, width), 1)
        == width - 1,
        1.0,
        0.0,
    ).astype(BF16)
    own_f.wait()
    for i in range(fd):
        for y in range(height):
            fwin[fd + i, RADIUS + y] = dot(flip, fsrc[y, i]).astype(BF16)
    pl.semaphore_wait(barrier, count)

    feats = {}
    edge_src = {UP: pl.ds(RADIUS, RADIUS), DOWN: pl.ds(height, RADIUS)}
    edge_dst = {UP: pl.ds(RADIUS + height, RADIUS), DOWN: pl.ds(0, RADIUS)}
    def offer(j):
        for way in (FAR, NEAR):
            feats[way, j] = push([
                (way, fwin.at[fd + j, own_rows], fwin.at[seat[way] + j, own_rows])
            ])

    offer(0)
    own_edges = push([
        (way, fwin.at[middle, edge_src[way]], fwin.at[middle, edge_dst[way]])
        for way in (UP, DOWN)
    ])

    line_src = {UP: 1, DOWN: height}
    line_dst = {UP: height + 1, DOWN: 0}
    own_c.wait()
    ctx_edges = push([
        (way, st.at[0, :, line_src[way]], st.at[0, :, line_dst[way]]) for way in (UP, DOWN)
    ])
    for j in range(1, fd):
        offer(j)

    fwin[:, 2 * RADIUS + height] = jnp.zeros((fwin.shape[0],) + fwin.shape[2:], BF16)
    for way, edge in ((UP, r == 0), (DOWN, r == nr - 1)):
        @pl.when(edge)
        def _(way=way):
            outside = back[way]
            fwin[:, edge_dst[outside]] = jnp.zeros(
                (fwin.shape[0], RADIUS, width, chans), BF16
            )
            line = line_dst[outside]
            mot[:, line] = jnp.zeros((total_combos, width, chans), BF16)
            hh[:, :, line] = jnp.zeros(hh.shape[:2] + (width, chans), BF16)
            st[0, :, line] = jnp.zeros((fd, width, chans), BF16)
            first = 0 if way == UP else height + 2
            ubuf[:, :, first : first + 2] = jnp.zeros((ROUNDS, fd, 2, width, chans), BF16)

    for way in (FAR, NEAR):
        @pl.when(jnp.logical_not(has[way]))
        def _(way=way):
            fwin[seat[way] : seat[way] + fd] = jnp.zeros((fd,) + fwin.shape[1:], BF16)
            for k in range(ROUNDS):
                mrecv[k, way] = jnp.zeros((fd, rows, chans), BF16)

    window = 3 * fd
    bases = [base * fd for base in (far, f, near)]
    codes = [i * window + j for _, _, _, members in groups for i, j in members]

    def tally(p, counts):
        i = pairs_s[0, p] - bases[1]
        own = jnp.logical_and(i >= 0, i < fd)
        code = jnp.int32(-1)
        for n, base in enumerate(bases):
            j = pairs_s[1, p] - base
            here = jnp.logical_and(own, jnp.logical_and(j >= 0, j < fd))
            code = jnp.where(here, i * window + n * fd + j, code)
        return tuple(v + (code == c).astype(jnp.int32) for v, c in zip(counts, codes))

    listed.wait()
    counts = lax.fori_loop(0, npair, tally, (jnp.int32(0),) * total_combos)
    for c in range(total_combos):
        tbl[c] = counts[c]

    def times(c):
        return tbl[c].astype(F32)

    per = LANES // width
    tiles = (SPAN + per - 1) // per
    depth = tiles * LANES
    origin = width - 1 - RADIUS

    def place(lane):
        spot = lax.rem(lane + (LANES - origin), LANES)
        return lax.div(spot, width), (SPAN - 1) - lax.rem(spot, width)

    corr_w.wait()
    line = lax.broadcasted_iota(jnp.int32, (depth, wcorr_s.shape[0]), 0)
    col = lax.broadcasted_iota(jnp.int32, (depth, wcorr_s.shape[0]), 1)
    half, b_off = place(lax.rem(line, LANES))
    a_off = lax.div(line, LANES) * per + half
    take = jnp.logical_and(b_off >= 0, a_off < SPAN)
    index = jnp.where(take, a_off * SPAN + b_off, -1)
    wsel[...] = dot(jnp.where(index == col, 1.0, 0.0).astype(BF16), wcorr_s[...]).astype(BF16)

    xs = lax.broadcasted_iota(jnp.int32, (width, LANES), 0)
    _, bs = place(lax.broadcasted_iota(jnp.int32, (width, LANES), 1))
    inside = jnp.logical_and(xs + bs >= RADIUS, xs + bs < width + RADIUS)
    inside = jnp.logical_and(inside, bs >= 0)
    scale = 1.0 / chans**0.5

    def banded(g):
        pieces = []
        for q in range(tiles):
            piece = pltpu.roll(g[:, q * LANES : (q + 1) * LANES], 0, 1, stride=1, stride_axis=0)
            pieces.append(jnp.where(inside, piece, 0.0).astype(BF16))
        return jnp.concatenate(pieces, axis=1)

    def correlate(group):
        correlate_rows(group)
        return edge_lines(group)

    def correlate_rows(group):
        way, _, start, members = group
        lines = [[] for _ in members]
        for y in range(height):
            if way is None:
                for n, (i, j) in enumerate(members):
                    b = fwin[j, y : y + tiles * per].reshape(tiles * per * width, chans)
                    lines[n].append(banded(dot_nt(fsrc[y, i], b)))
            else:
                j = members[0][1]
                b = fwin[j, y : y + tiles * per].reshape(tiles * per * width, chans)
                g = dot_nt(fsrc[y].reshape(fd * width, chans), b)
                for n in range(fd):
                    lines[n].append(banded(g[n * width : (n + 1) * width]))
        corr = jnp.concatenate([part for each in lines for part in each], axis=0)
        moved = jnp.maximum(dot(corr, wsel[...]) * scale, 0.0).astype(BF16)
        n = len(members)
        mot[start : start + n, 1 : height + 1] = moved.reshape(n, height, width, chans)

    def edge_lines(group):
        span = pl.ds(group[2], len(group[3]))
        return push([
            (side, mot.at[span, line_src[side]], mot.at[span, line_dst[side]])
            for side in (UP, DOWN)
        ])

    relays = {}

    def relay(j):
        for way in (FAR, NEAR):
            arrive(feats[way, j])
            spot = seat[way] + j
            relays[spot] = push(
                [
                    (side, fwin.at[spot, edge_src[side]], fwin.at[spot, edge_dst[side]])
                    for side in (UP, DOWN)
                ],
                gate=way,
            )

    def start_hidden(when):
        @pl.when(when)
        def _():
            arrive(ctx_edges)
            gate_w.wait()
            for i in range(fd):
                first = jnp.tanh(st[0, i].reshape(tall, chans).astype(F32))
                th[i] = first
                hw0[i] = dot(first.astype(BF16), wzr_s[0:chans])

    def compare_own(when):
        @pl.when(when)
        def _():
            arrive(own_edges)
            correlate_rows(groups[-1])

    even_row = lax.rem(r, 2) == 0
    compare_own(even_row)
    start_hidden(even_row)
    relay(0)
    compare_own(jnp.logical_not(even_row))
    mot_edges = {len(groups) - 1: edge_lines(groups[-1])}
    for j in range(1, fd):
        relay(j)
    start_hidden(jnp.logical_not(even_row))

    def compare(n):
        arrive(relays[groups[n][3][0][1]])
        mot_edges[n] = correlate(groups[n])

    remote = len(groups) - 1
    early = min(4, remote)
    for n in range(early):
        compare(n)
    for copy in late:
        copy.wait()

    def shifted_sum(acc):
        line_no = lax.rem(
            lax.broadcasted_iota(jnp.int32, (acc.shape[0], chans), 0), width
        )
        before = pltpu.roll(acc[:, 0:chans], 1, 0)
        after = pltpu.roll(acc[:, 2 * chans : 3 * chans], acc.shape[0] - 1, 0)
        return (
            jnp.where(line_no > 0, before, 0.0)
            + acc[:, chans : 2 * chans]
            + jnp.where(line_no < width - 1, after, 0.0)
        )

    gated = set()

    def gate(k, c, i):
        gated.add((k, c))
        state = st[k, i].reshape(tall, chans).astype(F32)
        xin = (mot[c].reshape(tall, chans).astype(F32) + state).astype(BF16)
        known = hw0[i] if k == 0 else hw[c]
        gates = dot(xin, wzr_s[chans : 2 * chans]) + known
        zbuf[c] = jax.nn.sigmoid(gates[width : width + rows, 0:chans])
        reset = jax.nn.sigmoid(gates[:, chans : 2 * chans])
        if k == 0:
            h = th[i]
        else:
            h = jnp.concatenate(
                [
                    hh[k - 1, c, 0].astype(F32), hid[c],
                    hh[k - 1, c, height + 1].astype(F32),
                ],
                axis=0,
            )
        qbuf[c, :, :, 0:chans] = (reset * h).astype(BF16).reshape(height + 2, width, chans)
        qbuf[c, :, :, chans : 2 * chans] = xin.reshape(height + 2, width, chans)

    def recur(k, group):
        _, _, start, members = group
        n = len(members)
        for m, (i, _) in enumerate(members):
            if (k, start + m) not in gated:
                gate(k, start + m, i)
        taps = [
            qbuf[start : start + n, t : t + height].reshape(n * rows, 2 * chans) for t in range(3)
        ]
        total = shifted_sum(dot(jnp.concatenate(taps, axis=1), wq_s[...]))
        for m, (i, j) in enumerate(members):
            c = start + m
            h = th[i, width : width + rows] if k == 0 else hid[c]
            z = zbuf[c]
            h = (1.0 - z) * h + z * jnp.tanh(total[m * rows : (m + 1) * rows])
            hid[c] = h
            if k < ROUNDS - 1:
                hh[k, c, 1 : height + 1] = h.astype(BF16).reshape(height, width, chans)
        if k < ROUNDS - 1:
            span = pl.ds(start, n)
            return push([
                (side, hh.at[k, span, line_src[side]], hh.at[k, span, line_dst[side]])
                for side in (UP, DOWN)
            ])
        return None

    def gather(members, start):
        total = None
        for c in range(start, start + len(members)):
            term = times(c) * hid[c]
            total = term if total is None else total + term
        return total

    hid_edges = {}
    for k in range(ROUNDS):
        parcels = {}
        for n, group in enumerate(groups):
            way, j, start, members = group
            if k == 0:
                if 0 < n <= remote - early:
                    compare(n + early - 1)
                arrive(mot_edges[n])
            if k > 0 and n == remote:
                last_ahead()
            hid_edges[n] = recur(k, group)
            if way is not None:
                msend[k, way, j] = gather(members, start).astype(BF16)
                parcels[way, j] = push([
                    (way, msend.at[k, way, j], mrecv.at[k, way, j])
                ])
        everything = [(c, m) for g in groups for c, m in enumerate(g[3], g[2])]
        for i in range(fd):
            first_sum = None
            second_sum = jnp.zeros((rows, chans), F32)
            for c, (s, t) in everything:
                if s == i:
                    term = times(c) * hid[c]
                    first_sum = term if first_sum is None else first_sum + term
                if t == fd + i:
                    second_sum = second_sum + times(c) * hid[c]
            mown[i] = dot(first_sum.astype(BF16), wmsg_s[0:chans])
            town[i] = second_sum

        def ahead(n, k=k, edges=dict(hid_edges)):
            _, _, start, members = groups[n]
            arrive(edges[n])
            for m in range(len(members)):
                c = start + m
                hw[c] = dot(hh[k, c].reshape(tall, chans), wzr_s[0:chans])

        reach = 2 if k < ROUNDS - 1 else 1
        lines = height + 2 * (reach - 1)
        u_src = {UP: pl.ds(2, reach), DOWN: pl.ds(height + 2 - reach, reach)}
        u_dst = {UP: pl.ds(height + 2, reach), DOWN: pl.ds(2 - reach, reach)}
        u_edges = {}

        def update(i):
            for way in (FAR, NEAR):
                arrive(parcels[way, i])
            arrived = mrecv[k, FAR, i].astype(F32) + mrecv[k, NEAR, i].astype(F32)
            second = (town[i] + arrived).astype(BF16)
            total = mown[i] + dot(second, wmsg_s[chans : 2 * chans])
            ubuf[k, i, 2 : height + 2] = (
                jnp.maximum(total, 0.0).astype(BF16).reshape(height, width, chans)
            )
            u_edges[i] = push([
                (side, ubuf.at[k, i, u_src[side]], ubuf.at[k, i, u_dst[side]])
                for side in (UP, DOWN)
            ])

        def inner(i):
            own = ubuf[k, i, 2 : height + 2].reshape(rows, chans)
            acc = dot(own, wres_s[chans : 2 * chans])
            blank = jnp.zeros((width, 3 * chans), F32)
            if height > 1:
                above = dot(own[: rows - width], wres_s[0:chans])
                below = dot(own[width:], wres_s[2 * chans : 3 * chans])
                acc = acc + jnp.concatenate([blank, above], axis=0)
                acc = acc + jnp.concatenate([below, blank], axis=0)
            old = st[k, i, 1 : height + 1].reshape(rows, chans)
            mown[i] = old.astype(F32) + shifted_sum(acc)

        def outer(i):
            arrive(u_edges[i])
            above = shifted_sum(dot(ubuf[k, i, 1], wres_s[0:chans]))
            below = shifted_sum(dot(ubuf[k, i, height + 2], wres_s[2 * chans : 3 * chans]))
            for y in range(height):
                total = mown[i, y * width : (y + 1) * width]
                if y == 0:
                    total = total + above
                if y == height - 1:
                    total = total + below
                out_ref[i, y] = total.astype(BF16)

        def residual(i):
            arrive(u_edges[i])
            taps = [
                ubuf[k, i, 2 - reach + t : 2 - reach + t + lines].reshape(lines * width, chans)
                for t in range(3)
            ]
            moved = shifted_sum(dot(jnp.concatenate(taps, axis=1), wres_s[...]))
            old = st[k, i].reshape(lines * width, chans)
            new = (old.astype(F32) + moved).astype(BF16).reshape(lines, width, chans)
            st[k + 1, i] = new
            for way, edge in ((UP, r == 0), (DOWN, r == nr - 1)):
                @pl.when(edge)
                def _(way=way):
                    st[k + 1, i, line_dst[back[way]]] = jnp.zeros((width, chans), BF16)

        for i in range(fd):
            update(i)
            if k < ROUNDS - 1:
                for n in range(i * remote // fd, (i + 1) * remote // fd):
                    ahead(n)
        if k == ROUNDS - 1:
            for i in range(fd):
                inner(i)
            for i in range(fd):
                outer(i)
        else:
            for i in range(fd):
                residual(i)
        last_ahead = functools.partial(ahead, remote)

    for kind, lines in sorted(sent.items()):
        way, gate = kinds[kind]

        @pl.when(both(has[way], None if gate is None else has[gate]))
        def _(way=way, kind=kind, lines=lines):
            part = bulk.at[pl.ds(0, lines)]
            rcopy(way, part, part, ssem.at[kind], rsem.at[0]).wait_send()


def local(nf, nr, fmap, context, pairs, w_corr, w_zr, w_q, w_msg, w_res):
    fd, height, width, chans = fmap.shape
    rows = height * width
    tall = rows + 2 * width
    win = 3 * fd
    groups, combos = plan(fd)
    tiles = -(-SPAN // (LANES // width))
    copies = 4 * fd + 2 + len(groups) * ROUNDS + ROUNDS * 3 * fd
    hbm = pl.BlockSpec(memory_space=pl.ANY)
    return pl.pallas_call(
        functools.partial(kernel, nf, nr),
        out_shape=pltpu.VMEM(fmap.shape, BF16),
        in_specs=[hbm] * 8,
        out_specs=pl.BlockSpec(memory_space=pltpu.VMEM),
        scratch_shapes=[
            pltpu.VMEM((height, fd, width, chans), BF16),
            pltpu.VMEM((win, 2 * RADIUS + height + 1, width, chans), BF16),
            pltpu.VMEM((ROUNDS, fd, height + 2, width, chans), BF16),
            pltpu.VMEM((combos, height + 2, width, chans), BF16),
            pltpu.VMEM((combos, rows, chans), F32),
            pltpu.VMEM((ROUNDS - 1, combos, height + 2, width, chans), BF16),
            pltpu.VMEM((fd, tall, chans), F32),
            pltpu.VMEM((fd, tall, 2 * chans), F32),
            pltpu.VMEM((combos, tall, 2 * chans), F32),
            pltpu.VMEM((combos, height + 2, width, 2 * chans), BF16),
            pltpu.VMEM((combos, rows, chans), F32),
            pltpu.VMEM((ROUNDS, 2, fd, rows, chans), BF16),
            pltpu.VMEM((ROUNDS, 2, fd, rows, chans), BF16),
            pltpu.VMEM((ROUNDS, fd, height + 4, width, chans), BF16),
            pltpu.VMEM((fd, rows, chans), F32),
            pltpu.VMEM((fd, rows, chans), F32),
            pltpu.VMEM((ROUNDS * (combos + 2 * fd) + 4 * fd, width, chans), BF16),
            pltpu.SMEM((3, pairs.shape[0]), jnp.int32),
            pltpu.VMEM(w_corr.shape, BF16),
            pltpu.VMEM((tiles * LANES, chans), BF16),
            pltpu.VMEM(w_zr.shape, BF16),
            pltpu.VMEM((6 * chans, 3 * chans), BF16),
            pltpu.VMEM((3 * chans, 3 * chans), BF16),
            pltpu.VMEM((2 * chans, chans), BF16),
            pltpu.SMEM((combos,), jnp.int32),
            pltpu.SemaphoreType.DMA((8,)),
            pltpu.SemaphoreType.DMA((copies,)),
            pltpu.SemaphoreType.DMA((8,)),
        ],
        compiler_params=pltpu.CompilerParams(collective_id=0, has_side_effects=True),
    )(pairs.T, fmap, context, w_corr, w_zr, w_q, w_msg, w_res)


def solution(mesh):
    placed = (P("frames", "rows", None, None), P("frames", "rows", None, None)) + (P(),) * 6
    return jax.shard_map(
        functools.partial(local, mesh.shape["frames"], mesh.shape["rows"]),
        mesh=mesh,
        in_specs=placed,
        out_specs=P("frames", "rows", None, None),
        check_vma=False,
    )
```

```python
import functools
import math

import jax
import jax.numpy as jnp
from jax import lax
from jax.experimental import pallas as pl
from jax.experimental.pallas import tpu as pltpu
from jax.sharding import PartitionSpec as P

RADIUS = 3
ROUNDS = 2
LANES = 128
SPAN = 2 * RADIUS + 1
MESH = pl.DeviceIdType.MESH
F32 = jnp.float32
BF16 = jnp.bfloat16
FAR, NEAR, UP, DOWN = range(4)


def dot(a, b):
    return jnp.dot(a, b, preferred_element_type=F32)


def dot_nt(a, b):
    return lax.dot_general(a, b, (((1,), (1,)), ((), ())), preferred_element_type=F32)


def plan(fd):
    groups = []
    for j in range(fd):
        for way, seat in ((FAR, j), (NEAR, 2 * fd + j)):
            groups.append((way, j, [(i, seat) for i in range(fd)]))
    groups.append((None, 0, [(i, fd + j) for j in range(fd) for i in range(fd) if i != j]))
    start = 0
    out = []
    for way, j, members in groups:
        out.append((way, j, start, members))
        start += len(members)
    return out, start


def kernel(
    nf, nr,
    pairs_ref, fmap_ref, ctx_ref, wcorr_ref, wzr_ref, wq_ref, wmsg_ref, wres_ref,
    out_ref,
    fsrc, fwin, st, mot, hid, hh, th, hw0, hw, qbuf, zbuf,
    msend, mrecv, ubuf, mown, town,
    bulk, pairs_s, wcorr_s, wsel, wzr_s, wq_s, wres_s, wmsg_s, tbl,
    ssem, rsem, lsem,
):
    f = lax.axis_index("frames")
    r = lax.axis_index("rows")
    height, fd, width, chans = fsrc.shape
    npair = pairs_ref.shape[1]
    rows = height * width
    tall = (height + 2) * width
    groups, total_combos = plan(fd)
    step = 1 - 2 * lax.rem(f, 2)
    near, far = f + step, f - step
    has = {
        FAR: jnp.logical_and(far >= 0, far < nf), NEAR: jnp.logical_and(near >= 0, near < nf),
        UP: r > 0, DOWN: r < nr - 1,
    }
    dev = {FAR: (far, r), NEAR: (near, r), UP: (f, r - 1), DOWN: (f, r + 1)}
    back = {FAR: FAR, NEAR: NEAR, UP: DOWN, DOWN: UP}
    sent = {}
    landed = []

    def both(cond, gate):
        return cond if gate is None else jnp.logical_and(cond, gate)

    def rcopy(way, src, dst, send_sem, recv_sem):
        return pltpu.make_async_remote_copy(
            src_ref=src, dst_ref=dst, send_sem=send_sem, recv_sem=recv_sem,
            device_id=dev[way], device_id_type=MESH,
        )

    def lines_of(ref):
        return math.prod(ref.shape) // (width * chans)

    kinds = [(way, None) for way in (FAR, NEAR, UP, DOWN)]
    kinds += [(side, way) for side in (UP, DOWN) for way in (FAR, NEAR)]

    def push(copies, gate=None):
        spot = len(landed)
        landed.append(None)
        for way, src, dst in copies:
            kind = kinds.index((way, gate))
            sent[kind] = sent.get(kind, 0) + lines_of(src)

            @pl.when(both(has[way], None if gate is None else has[gate]))
            def _(way=way, src=src, dst=dst, kind=kind):
                rcopy(way, src, dst, ssem.at[kind], rsem.at[spot]).start()

        return spot, [way for way, _, _ in copies], lines_of(copies[0][1]), gate

    def await_lines(way, spot, lines):
        part = bulk.at[pl.ds(0, lines)]
        rcopy(way, part, part, ssem.at[0], rsem.at[spot]).wait_recv()

    def arrive(handle):
        spot, ways, lines, gate = handle
        gate = None if gate is None else has[gate]
        if len(ways) == 1:
            @pl.when(both(has[back[ways[0]]], gate))
            def _():
                await_lines(ways[0], spot, lines)
        else:
            here, there = (has[back[way]] for way in ways)

            @pl.when(both(jnp.logical_and(here, there), gate))
            def _():
                await_lines(ways[0], spot, 2 * lines)

            @pl.when(both(jnp.not_equal(here, there), gate))
            def _():
                await_lines(ways[0], spot, lines)

    own_rows = pl.ds(RADIUS, height)
    middle = pl.ds(fd, fd)
    seat = {FAR: 0, NEAR: 2 * fd}

    class Load:
        def __init__(self, n, whole, copies):
            self.n, self.whole = n, whole
            for src, dst in copies:
                pltpu.make_async_copy(src, dst, lsem.at[n]).start()

        def wait(self):
            pltpu.make_async_copy(self.whole, self.whole, lsem.at[self.n]).wait()

    def lanes(j):
        return pl.ds(j * chans, chans)

    taps = [(k, j) for k in range(3) for j in range(3)]
    own_f = Load(0, fsrc, [(fmap_ref.at[i], fsrc.at[:, i]) for i in range(fd)])
    barrier = pltpu.get_barrier_semaphore()
    count = 0
    for way in (FAR, NEAR, UP, DOWN):
        count = count + has[way].astype(jnp.int32)

        @pl.when(has[way])
        def _(way=way):
            pl.semaphore_signal(barrier, inc=1, device_id=dev[way], device_id_type=MESH)

    own_c = pltpu.make_async_copy(ctx_ref, st.at[0, :, pl.ds(1, height)], lsem.at[1])
    own_c.start()
    listed = Load(2, pairs_s, [(pairs_ref, pairs_s)])
    corr_w = Load(3, wcorr_s, [(wcorr_ref, wcorr_s)])
    gate_w = Load(4, wzr_s, [(wzr_ref, wzr_s)])
    late = [
        Load(5, wq_s, [
            (wq_ref.at[3 * k + j], wq_s.at[pl.ds(2 * k * chans, 2 * chans), lanes(j)])
            for k, j in taps
        ]),
        Load(6, wres_s, [
            (wres_ref.at[3 * k + j], wres_s.at[lanes(k), lanes(j)]) for k, j in taps
        ]),
        Load(7, wmsg_s, [(wmsg_ref.at[:, lanes(k)], wmsg_s.at[lanes(k)]) for k in range(2)]),
    ]

    flip = jnp.where(
        lax.broadcasted_iota(jnp.int32, (width, width), 0)
        + lax.broadcasted_iota(jnp.int32, (width, width), 1)
        == width - 1,
        1.0,
        0.0,
    ).astype(BF16)
    own_f.wait()
    for i in range(fd):
        for y in range(height):
            fwin[fd + i, RADIUS + y] = dot(flip, fsrc[y, i]).astype(BF16)
    pl.semaphore_wait(barrier, count)

    feats = {}
    edge_src = {UP: pl.ds(RADIUS, RADIUS), DOWN: pl.ds(height, RADIUS)}
    edge_dst = {UP: pl.ds(RADIUS + height, RADIUS), DOWN: pl.ds(0, RADIUS)}
    def offer(j):
        for way in (FAR, NEAR):
            feats[way, j] = push([
                (way, fwin.at[fd + j, own_rows], fwin.at[seat[way] + j, own_rows])
            ])

    offer(0)
    own_edges = push([
        (way, fwin.at[middle, edge_src[way]], fwin.at[middle, edge_dst[way]])
        for way in (UP, DOWN)
    ])

    line_src = {UP: 1, DOWN: height}
    line_dst = {UP: height + 1, DOWN: 0}
    own_c.wait()
    ctx_edges = push([
        (way, st.at[0, :, line_src[way]], st.at[0, :, line_dst[way]]) for way in (UP, DOWN)
    ])
    for j in range(1, fd):
        offer(j)

    fwin[:, 2 * RADIUS + height] = jnp.zeros((fwin.shape[0],) + fwin.shape[2:], BF16)
    for way, edge in ((UP, r == 0), (DOWN, r == nr - 1)):
        @pl.when(edge)
        def _(way=way):
            outside = back[way]
            fwin[:, edge_dst[outside]] = jnp.zeros(
                (fwin.shape[0], RADIUS, width, chans), BF16
            )
            line = line_dst[outside]
            mot[:, line] = jnp.zeros((total_combos, width, chans), BF16)
            hh[:, :, line] = jnp.zeros(hh.shape[:2] + (width, chans), BF16)
            st[0, :, line] = jnp.zeros((fd, width, chans), BF16)
            first = 0 if way == UP else height + 2
            ubuf[:, :, first : first + 2] = jnp.zeros((ROUNDS, fd, 2, width, chans), BF16)

    for way in (FAR, NEAR):
        @pl.when(jnp.logical_not(has[way]))
        def _(way=way):
            fwin[seat[way] : seat[way] + fd] = jnp.zeros((fd,) + fwin.shape[1:], BF16)
            for k in range(ROUNDS):
                mrecv[k, way] = jnp.zeros((fd, rows, chans), BF16)

    window = 3 * fd
    bases = [base * fd for base in (far, f, near)]
    codes = [i * window + j for _, _, _, members in groups for i, j in members]

    def tally(p, counts):
        i = pairs_s[0, p] - bases[1]
        own = jnp.logical_and(i >= 0, i < fd)
        code = jnp.int32(-1)
        for n, base in enumerate(bases):
            j = pairs_s[1, p] - base
            here = jnp.logical_and(own, jnp.logical_and(j >= 0, j < fd))
            code = jnp.where(here, i * window + n * fd + j, code)
        return tuple(v + (code == c).astype(jnp.int32) for v, c in zip(counts, codes))

    listed.wait()
    counts = lax.fori_loop(0, npair, tally, (jnp.int32(0),) * total_combos)
    for c in range(total_combos):
        tbl[c] = counts[c]

    def times(c):
        return tbl[c].astype(F32)

    per = LANES // width
    tiles = (SPAN + per - 1) // per
    depth = tiles * LANES
    origin = width - 1 - RADIUS

    def place(lane):
        spot = lax.rem(lane + (LANES - origin), LANES)
        return lax.div(spot, width), (SPAN - 1) - lax.rem(spot, width)

    corr_w.wait()
    line = lax.broadcasted_iota(jnp.int32, (depth, wcorr_s.shape[0]), 0)
    col = lax.broadcasted_iota(jnp.int32, (depth, wcorr_s.shape[0]), 1)
    half, b_off = place(lax.rem(line, LANES))
    a_off = lax.div(line, LANES) * per + half
    take = jnp.logical_and(b_off >= 0, a_off < SPAN)
    index = jnp.where(take, a_off * SPAN + b_off, -1)
    wsel[...] = dot(jnp.where(index == col, 1.0, 0.0).astype(BF16), wcorr_s[...]).astype(BF16)

    xs = lax.broadcasted_iota(jnp.int32, (width, LANES), 0)
    _, bs = place(lax.broadcasted_iota(jnp.int32, (width, LANES), 1))
    inside = jnp.logical_and(xs + bs >= RADIUS, xs + bs < width + RADIUS)
    inside = jnp.logical_and(inside, bs >= 0)
    scale = 1.0 / chans**0.5

    def banded(g):
        pieces = []
        for q in range(tiles):
            piece = pltpu.roll(g[:, q * LANES : (q + 1) * LANES], 0, 1, stride=1, stride_axis=0)
            pieces.append(jnp.where(inside, piece, 0.0).astype(BF16))
        return jnp.concatenate(pieces, axis=1)

    def correlate(group):
        correlate_rows(group)
        return edge_lines(group)

    def correlate_rows(group):
        way, _, start, members = group
        lines = [[] for _ in members]
        for y in range(height):
            if way is None:
                for n, (i, j) in enumerate(members):
                    b = fwin[j, y : y + tiles * per].reshape(tiles * per * width, chans)
                    lines[n].append(banded(dot_nt(fsrc[y, i], b)))
            else:
                j = members[0][1]
                b = fwin[j, y : y + tiles * per].reshape(tiles * per * width, chans)
                g = dot_nt(fsrc[y].reshape(fd * width, chans), b)
                for n in range(fd):
                    lines[n].append(banded(g[n * width : (n + 1) * width]))
        corr = jnp.concatenate([part for each in lines for part in each], axis=0)
        moved = jnp.maximum(dot(corr, wsel[...]) * scale, 0.0).astype(BF16)
        n = len(members)
        mot[start : start + n, 1 : height + 1] = moved.reshape(n, height, width, chans)

    def edge_lines(group):
        span = pl.ds(group[2], len(group[3]))
        return push([
            (side, mot.at[span, line_src[side]], mot.at[span, line_dst[side]])
            for side in (UP, DOWN)
        ])

    relays = {}

    def relay(j):
        for way in (FAR, NEAR):
            arrive(feats[way, j])
            spot = seat[way] + j
            relays[spot] = push(
                [
                    (side, fwin.at[spot, edge_src[side]], fwin.at[spot, edge_dst[side]])
                    for side in (UP, DOWN)
                ],
                gate=way,
            )

    def start_hidden(when):
        @pl.when(when)
        def _():
            arrive(ctx_edges)
            gate_w.wait()
            for i in range(fd):
                first = jnp.tanh(st[0, i].reshape(tall, chans).astype(F32))
                th[i] = first
                hw0[i] = dot(first.astype(BF16), wzr_s[0:chans])

    def compare_own(when):
        @pl.when(when)
        def _():
            arrive(own_edges)
            correlate_rows(groups[-1])

    even_row = lax.rem(r, 2) == 0
    compare_own(even_row)
    start_hidden(even_row)
    relay(0)
    compare_own(jnp.logical_not(even_row))
    mot_edges = {len(groups) - 1: edge_lines(groups[-1])}
    for j in range(1, fd):
        relay(j)
    start_hidden(jnp.logical_not(even_row))

    def compare(n):
        arrive(relays[groups[n][3][0][1]])
        mot_edges[n] = correlate(groups[n])

    remote = len(groups) - 1
    early = min(4, remote)
    for n in range(early):
        compare(n)
    for copy in late:
        copy.wait()

    def shifted_sum(acc):
        line_no = lax.rem(
            lax.broadcasted_iota(jnp.int32, (acc.shape[0], chans), 0), width
        )
        before = pltpu.roll(acc[:, 0:chans], 1, 0)
        after = pltpu.roll(acc[:, 2 * chans : 3 * chans], acc.shape[0] - 1, 0)
        return (
            jnp.where(line_no > 0, before, 0.0)
            + acc[:, chans : 2 * chans]
            + jnp.where(line_no < width - 1, after, 0.0)
        )

    gated = set()

    def gate(k, c, i):
        gated.add((k, c))
        state = st[k, i].reshape(tall, chans).astype(F32)
        xin = (mot[c].reshape(tall, chans).astype(F32) + state).astype(BF16)
        known = hw0[i] if k == 0 else hw[c]
        gates = dot(xin, wzr_s[chans : 2 * chans]) + known
        zbuf[c] = jax.nn.sigmoid(gates[width : width + rows, 0:chans])
        reset = jax.nn.sigmoid(gates[:, chans : 2 * chans])
        if k == 0:
            h = th[i]
        else:
            h = jnp.concatenate(
                [
                    hh[k - 1, c, 0].astype(F32), hid[c],
                    hh[k - 1, c, height + 1].astype(F32),
                ],
                axis=0,
            )
        qbuf[c, :, :, 0:chans] = (reset * h).astype(BF16).reshape(height + 2, width, chans)
        qbuf[c, :, :, chans : 2 * chans] = xin.reshape(height + 2, width, chans)

    def recur(k, group):
        _, _, start, members = group
        n = len(members)
        for m, (i, _) in enumerate(members):
            if (k, start + m) not in gated:
                gate(k, start + m, i)
        taps = [
            qbuf[start : start + n, t : t + height].reshape(n * rows, 2 * chans) for t in range(3)
        ]
        total = shifted_sum(dot(jnp.concatenate(taps, axis=1), wq_s[...]))
        for m, (i, j) in enumerate(members):
            c = start + m
            h = th[i, width : width + rows] if k == 0 else hid[c]
            z = zbuf[c]
            h = (1.0 - z) * h + z * jnp.tanh(total[m * rows : (m + 1) * rows])
            hid[c] = h
            if k < ROUNDS - 1:
                hh[k, c, 1 : height + 1] = h.astype(BF16).reshape(height, width, chans)
        if k < ROUNDS - 1:
            span = pl.ds(start, n)
            return push([
                (side, hh.at[k, span, line_src[side]], hh.at[k, span, line_dst[side]])
                for side in (UP, DOWN)
            ])
        return None

    def gather(members, start):
        total = None
        for c in range(start, start + len(members)):
            term = times(c) * hid[c]
            total = term if total is None else total + term
        return total

    hid_edges = {}
    for k in range(ROUNDS):
        parcels = {}
        for n, group in enumerate(groups):
            way, j, start, members = group
            if k == 0:
                if 0 < n <= remote - early:
                    compare(n + early - 1)
                arrive(mot_edges[n])
            if k > 0 and n == remote:
                last_ahead()
            hid_edges[n] = recur(k, group)
            if way is not None:
                msend[k, way, j] = gather(members, start).astype(BF16)
                parcels[way, j] = push([
                    (way, msend.at[k, way, j], mrecv.at[k, way, j])
                ])
        everything = [(c, m) for g in groups for c, m in enumerate(g[3], g[2])]
        for i in range(fd):
            first_sum = None
            second_sum = jnp.zeros((rows, chans), F32)
            for c, (s, t) in everything:
                if s == i:
                    term = times(c) * hid[c]
                    first_sum = term if first_sum is None else first_sum + term
                if t == fd + i:
                    second_sum = second_sum + times(c) * hid[c]
            mown[i] = dot(first_sum.astype(BF16), wmsg_s[0:chans])
            town[i] = second_sum

        def ahead(n, k=k, edges=dict(hid_edges)):
            _, _, start, members = groups[n]
            arrive(edges[n])
            for m in range(len(members)):
                c = start + m
                hw[c] = dot(hh[k, c].reshape(tall, chans), wzr_s[0:chans])

        reach = 2 if k < ROUNDS - 1 else 1
        lines = height + 2 * (reach - 1)
        u_src = {UP: pl.ds(2, reach), DOWN: pl.ds(height + 2 - reach, reach)}
        u_dst = {UP: pl.ds(height + 2, reach), DOWN: pl.ds(2 - reach, reach)}
        u_edges = {}

        def update(i):
            for way in (FAR, NEAR):
                arrive(parcels[way, i])
            arrived = mrecv[k, FAR, i].astype(F32) + mrecv[k, NEAR, i].astype(F32)
            second = (town[i] + arrived).astype(BF16)
            total = mown[i] + dot(second, wmsg_s[chans : 2 * chans])
            ubuf[k, i, 2 : height + 2] = (
                jnp.maximum(total, 0.0).astype(BF16).reshape(height, width, chans)
            )
            u_edges[i] = push([
                (side, ubuf.at[k, i, u_src[side]], ubuf.at[k, i, u_dst[side]])
                for side in (UP, DOWN)
            ])

        def inner(i):
            own = ubuf[k, i, 2 : height + 2].reshape(rows, chans)
            acc = dot(own, wres_s[chans : 2 * chans])
            blank = jnp.zeros((width, 3 * chans), F32)
            if height > 1:
                above = dot(own[: rows - width], wres_s[0:chans])
                below = dot(own[width:], wres_s[2 * chans : 3 * chans])
                acc = acc + jnp.concatenate([blank, above], axis=0)
                acc = acc + jnp.concatenate([below, blank], axis=0)
            old = st[k, i, 1 : height + 1].reshape(rows, chans)
            mown[i] = old.astype(F32) + shifted_sum(acc)

        def outer(i):
            arrive(u_edges[i])
            above = shifted_sum(dot(ubuf[k, i, 1], wres_s[0:chans]))
            below = shifted_sum(dot(ubuf[k, i, height + 2], wres_s[2 * chans : 3 * chans]))
            for y in range(height):
                total = mown[i, y * width : (y + 1) * width]
                if y == 0:
                    total = total + above
                if y == height - 1:
                    total = total + below
                out_ref[i, y] = total.astype(BF16)

        def residual(i):
            arrive(u_edges[i])
            taps = [
                ubuf[k, i, 2 - reach + t : 2 - reach + t + lines].reshape(lines * width, chans)
                for t in range(3)
            ]
            moved = shifted_sum(dot(jnp.concatenate(taps, axis=1), wres_s[...]))
            old = st[k, i].reshape(lines * width, chans)
            new = (old.astype(F32) + moved).astype(BF16).reshape(lines, width, chans)
            st[k + 1, i] = new
            for way, edge in ((UP, r == 0), (DOWN, r == nr - 1)):
                @pl.when(edge)
                def _(way=way):
                    st[k + 1, i, line_dst[back[way]]] = jnp.zeros((width, chans), BF16)

        for i in range(fd):
            update(i)
            if k < ROUNDS - 1:
                for n in range(i * remote // fd, (i + 1) * remote // fd):
                    ahead(n)
        if k == ROUNDS - 1:
            for i in range(fd):
                inner(i)
            for i in range(fd):
                outer(i)
        else:
            for i in range(fd):
                residual(i)
        last_ahead = functools.partial(ahead, remote)

    for kind, lines in sorted(sent.items()):
        way, gate = kinds[kind]

        @pl.when(both(has[way], None if gate is None else has[gate]))
        def _(way=way, kind=kind, lines=lines):
            part = bulk.at[pl.ds(0, lines)]
            rcopy(way, part, part, ssem.at[kind], rsem.at[0]).wait_send()


def local(nf, nr, fmap, context, pairs, w_corr, w_zr, w_q, w_msg, w_res):
    fd, height, width, chans = fmap.shape
    rows = height * width
    tall = rows + 2 * width
    win = 3 * fd
    groups, combos = plan(fd)
    tiles = -(-SPAN // (LANES // width))
    copies = 4 * fd + 2 + len(groups) * ROUNDS + ROUNDS * 3 * fd
    hbm = pl.BlockSpec(memory_space=pl.ANY)
    return pl.pallas_call(
        functools.partial(kernel, nf, nr),
        out_shape=pltpu.VMEM(fmap.shape, BF16),
        in_specs=[hbm] * 8,
        out_specs=pl.BlockSpec(memory_space=pltpu.VMEM),
        scratch_shapes=[
            pltpu.VMEM((height, fd, width, chans), BF16),
            pltpu.VMEM((win, 2 * RADIUS + height + 1, width, chans), BF16),
            pltpu.VMEM((ROUNDS, fd, height + 2, width, chans), BF16),
            pltpu.VMEM((combos, height + 2, width, chans), BF16),
            pltpu.VMEM((combos, rows, chans), F32),
            pltpu.VMEM((ROUNDS - 1, combos, height + 2, width, chans), BF16),
            pltpu.VMEM((fd, tall, chans), F32),
            pltpu.VMEM((fd, tall, 2 * chans), F32),
            pltpu.VMEM((combos, tall, 2 * chans), F32),
            pltpu.VMEM((combos, height + 2, width, 2 * chans), BF16),
            pltpu.VMEM((combos, rows, chans), F32),
            pltpu.VMEM((ROUNDS, 2, fd, rows, chans), BF16),
            pltpu.VMEM((ROUNDS, 2, fd, rows, chans), BF16),
            pltpu.VMEM((ROUNDS, fd, height + 4, width, chans), BF16),
            pltpu.VMEM((fd, rows, chans), F32),
            pltpu.VMEM((fd, rows, chans), F32),
            pltpu.VMEM((ROUNDS * (combos + 2 * fd) + 4 * fd, width, chans), BF16),
            pltpu.SMEM((3, pairs.shape[0]), jnp.int32),
            pltpu.VMEM(w_corr.shape, BF16),
            pltpu.VMEM((tiles * LANES, chans), BF16),
            pltpu.VMEM(w_zr.shape, BF16),
            pltpu.VMEM((6 * chans, 3 * chans), BF16),
            pltpu.VMEM((3 * chans, 3 * chans), BF16),
            pltpu.VMEM((2 * chans, chans), BF16),
            pltpu.SMEM((combos,), jnp.int32),
            pltpu.SemaphoreType.DMA((8,)),
            pltpu.SemaphoreType.DMA((copies,)),
            pltpu.SemaphoreType.DMA((8,)),
        ],
        compiler_params=pltpu.CompilerParams(
            collective_id=0, has_side_effects=True,
        ),
    )(pairs.T, fmap, context, w_corr, w_zr, w_q, w_msg, w_res)


def solution(mesh):
    placed = (P("frames", "rows", None, None), P("frames", "rows", None, None)) + (P(),) * 6
    return jax.shard_map(
        functools.partial(local, mesh.shape["frames"], mesh.shape["rows"]),
        mesh=mesh,
        in_specs=placed,
        out_specs=P("frames", "rows", None, None),
        check_vma=False,
    )
```
